32 devices in a mesh: dp: 8 (over y, x, core), expert: 4 (over z).
Axes of the slice: x: 2, y: 2, z: 4, core: 2. Of those that a mesh axis runs over, the one named last changes fastest.
Arguments:
- tokens: bfloat16 [4096, 2048], P(('dp', 'expert')), may hold values from -6 to 6
- cotangent: bfloat16 [4096, 2048], P(('dp', 'expert')), may hold values from -6 to 6
- expert_ids: int32 [4096, 2], P(('dp', 'expert')), may hold values from 0 to 3, all different within a row; in each aligned block of 128 rows (0 to 127, 128 to 255, ...) at most 128 rows name the same one
- combine: float32 [4096, 2], P(('dp', 'expert')), may hold values from 0.1 to 1
- w_gate: bfloat16 [4, 2048, 768], P('expert'), may hold values from -0.125 to 0.125
- w_up: bfloat16 [4, 2048, 768], P('expert'), may hold values from -0.125 to 0.125
- w_down: bfloat16 [4, 768, 2048], P('expert'), may hold values from -0.21875 to 0.21875
Outputs:
- input_grad: bfloat16 [4096, 2048], P(('dp', 'expert'))
- combine_grad: float32 [4096, 2], P(('dp', 'expert'))
- gate_grad: bfloat16 [4, 2048, 768], P('expert', 'dp')
- up_grad: bfloat16 [4, 2048, 768], P('expert', 'dp')
- down_grad: bfloat16 [4, 768, 2048], P('expert', 'dp')
The draws below stay inside these ranges and needn't reach their ends.
Inputs may be any that keep to these rules, and one draw needn't show every extreme that they name: `expert_ids`: each token names 2 different experts. In the rows of one device no expert is named by more than 128 tokens, and in some devices' rows some expert is named by exactly 128.
All inputs are finite; a program needn't handle non-finite values.
Results may differ from the reference program's by a relative error of at most 0.02.
Values may be sent and summed in bfloat16 or wider, within the bound.
A program may use at most 128 MiB of HBM per device.

```python
import math
import jax
import jax.numpy as jnp
import numpy as np
from jax import lax

D = 2048
FF = 768
TOK_DEV = 128
TOP = 2
EXPERTS = 4
CAP = 128
TOKENS = 4096
N_DP = 8
N_EXPERT = 4


def steps_of(own_key, shape, split, smallest, largest):
    gain, own = 1.0, jax.random.fold_in(own_key, 6)
    for axis_at, parts in split:
        heights = jnp.exp(jax.random.uniform(jax.random.fold_in(own, axis_at), (parts,), jnp.float32, smallest / len(split), largest / len(split)))
        gain = gain * jnp.repeat(heights, shape[axis_at] // parts).reshape([-1 if axis == axis_at else 1 for axis in range(len(shape))])
    return gain


def deal_out(own_key, own, number, rows, number_of, top, bound, skew):
    ranking = jax.random.permutation(own_key, number_of)
    crowded, common = load_shares(number_of, rows * top, bound, skew, True), load_shares(number_of, rows * top, bound, skew, False)
    places = jnp.arange(number_of)

    def named(lengths, offset_by):
        used = int((lengths > 0).sum())
        fixed = max(1, used // 4)
        shifted = fixed + (places - fixed + offset_by * (used - fixed)) % max(1, number_of - fixed)
        return jnp.zeros((number_of,), jnp.int32).at[ranking[jnp.where(places < fixed, places, shifted)]].set(jnp.asarray(lengths, jnp.int32))

    lengths = jnp.where(number % 4 == 0, named(crowded, number // 4), named(common, number - number // 4 - 1))
    mixed = jax.random.permutation(jax.random.fold_in(own, 3), number_of)
    donor, taker = mixed[0:number_of // 2 * 2:2], mixed[1:number_of // 2 * 2:2]
    room = jnp.minimum(lengths[donor] - 1, bound - lengths[taker]) // 2
    room = jnp.where((donor == ranking[0]) | (taker == ranking[0]) | (lengths[taker] == 0), 0, jnp.maximum(room, 0))
    shifted = jax.random.randint(jax.random.fold_in(own, 4), (number_of // 2,), 0, 1 << 20) % (room + 1)
    lengths = lengths.at[donor].add(-shifted).at[taker].add(shifted)
    items = jnp.searchsorted(jnp.cumsum(lengths), jnp.arange(rows * top), side="right").astype(jnp.int32)
    listing = items.reshape(top, rows).T
    listing = listing[jax.random.permutation(jax.random.fold_in(own, 1), rows)]
    offset_by = jax.random.randint(jax.random.fold_in(own, 2), (rows, 1), 0, top)
    return jnp.take_along_axis(listing, (jnp.arange(top)[None, :] + offset_by) % top, axis=1)


def load_shares(number_of, total, bound, skew, full):
    weights = [(1 << 20) // math.isqrt(standing ** skew) + 1 for standing in range(1, number_of + 1)]
    largest = bound if full else min(bound, max(-(-total // number_of), total * weights[0] // sum(weights)))
    least = 1 if total - largest >= number_of - 1 else 0
    holding, spare = [largest] + [least] * (number_of - 1), total - largest - least * (number_of - 1)
    while spare > 0:
        candidates = [i for i in range(1, number_of) if holding[i] < largest] or [i for i in range(1, number_of) if holding[i] < bound]
        mass, left = sum([weights[i] for i in candidates]), spare
        for i in candidates:
            more = min(bound - holding[i], max(1, left * weights[i] // mass), spare)
            holding[i] = holding[i] + more
            spare = spare - more
    return np.array(holding)


def noise(rng, shape, deviation, reach, split=(), kind=jnp.bfloat16):
    result = jax.random.normal(rng, shape, jnp.float32) * deviation
    if len(split) > 0:
        result = steps_of(rng, shape, split, -0.22, 0.18) * result
    return jnp.clip(result, min=-reach, max=reach).astype(kind)


def setup_inputs(seed: int = 0) -> dict:
    key_list = jax.random.split(jax.random.key(seed), 8)
    tokens = noise(key_list[0], (TOKENS, D), 1.0, 6.0, ((0, 32),))
    cotangent = noise(key_list[1], (TOKENS, D), 1.0, 6.0, ((0, 32),))
    expert_ids_keys = jax.random.split(jax.random.fold_in(key_list[2], 1), TOKENS // TOK_DEV)
    expert_ids_turns = jax.random.permutation(jax.random.fold_in(key_list[2], 3), TOKENS // TOK_DEV)
    expert_ids = jax.vmap(lambda own, number: deal_out(jax.random.fold_in(key_list[2], 2), own, number, TOK_DEV, EXPERTS, TOP, CAP, 2))(expert_ids_keys, expert_ids_turns).reshape((TOKENS, TOP))
    combine = jnp.clip(jnp.exp(math.log(1.0) - 2.3025851 * jax.random.uniform(key_list[3], (TOKENS, TOP), jnp.float32) ** steps_of(key_list[3], (TOKENS, TOP), ((0, 32),), -0.2, 0.2)), 0.1, 1.0)
    w_gate = noise(key_list[4], (EXPERTS, D, FF), D ** -0.5, 0.125, ((0, 4),))
    w_up = noise(key_list[5], (EXPERTS, D, FF), D ** -0.5, 0.125, ((0, 4),))
    w_down = noise(key_list[6], (EXPERTS, FF, D), FF ** -0.5, 0.21875, ((0, 4),))
    return dict(tokens=tokens, cotangent=cotangent, expert_ids=expert_ids, combine=combine, w_gate=w_gate, w_up=w_up, w_down=w_down)


def slot_table(expert_ids, experts_all, capacity):
    pairs = expert_ids.reshape(-1).astype(jnp.int32)
    count = pairs.shape[0]
    onehot = (pairs[:, None] == jnp.arange(experts_all, dtype=jnp.int32)[None, :]).astype(jnp.int32)
    before = jnp.cumsum(onehot, axis=0) - onehot
    position = jnp.sum(before * onehot, axis=1).astype(jnp.int32)
    dest = (pairs * capacity + position).astype(jnp.int32)
    filled = jnp.zeros((experts_all * capacity,), jnp.int32).at[dest].set(jnp.arange(count, dtype=jnp.int32) + 1)
    return dest, filled


def gather_rows(tokens, cotangent, combine, filled, top):
    live = filled > 0
    pair = jnp.maximum(filled - 1, 0).astype(jnp.int32)
    source = (pair // top).astype(jnp.int32)
    rows_x = jnp.where(live[:, None], jnp.take(tokens, source, axis=0), jnp.zeros((), tokens.dtype))
    rows_dy = jnp.where(live[:, None], jnp.take(cotangent, source, axis=0), jnp.zeros((), cotangent.dtype))
    rows_c = jnp.where(live, jnp.take(combine.reshape(-1), pair, axis=0), jnp.zeros((), combine.dtype))
    return rows_x, rows_dy, rows_c


def forward_part(rows_x, gate_mat, up_mat, down_mat):
    gate = jnp.dot(rows_x, gate_mat, preferred_element_type=jnp.float32)
    up = jnp.dot(rows_x, up_mat, preferred_element_type=jnp.float32)
    sig = jax.nn.sigmoid(gate)
    act = gate * sig
    hidden = (act * up).astype(jnp.bfloat16)
    output = jnp.dot(hidden, down_mat, preferred_element_type=jnp.float32)
    return gate, up, sig, act, hidden, output


def backward_part(state, rows_dy, rows_c, gate_mat, up_mat, down_mat):
    gate, up, sig, act, hidden, output = state
    comb_grad = jnp.sum(rows_dy.astype(jnp.float32) * output, axis=1)
    scaled = (rows_c[:, None] * rows_dy.astype(jnp.float32)).astype(jnp.bfloat16)
    last = (((1,), (1,)), ((), ()))
    hidden_grad = lax.dot_general(scaled, down_mat, last, preferred_element_type=jnp.float32)
    gate_d = (hidden_grad * up * (sig * (1.0 + gate * (1.0 - sig)))).astype(jnp.bfloat16)
    up_d = (hidden_grad * act).astype(jnp.bfloat16)
    row_grad = lax.dot_general(gate_d, gate_mat, last, preferred_element_type=jnp.float32)
    row_grad = (row_grad + lax.dot_general(up_d, up_mat, last, preferred_element_type=jnp.float32)).astype(jnp.bfloat16)
    return comb_grad, scaled, gate_d, up_d, row_grad


def reference(tokens, cotangent, expert_ids, combine, w_gate, w_up, w_down):
    first = (((0,), (0,)), ((), ()))
    x_all = tokens.reshape(N_DP, N_EXPERT, TOK_DEV, D)
    dy_all = cotangent.reshape(N_DP, N_EXPERT, TOK_DEV, D)
    id_all = expert_ids.reshape(N_DP, N_EXPERT, TOK_DEV, TOP)
    c_all = combine.reshape(N_DP, N_EXPERT, TOK_DEV, TOP)

    def prepare(x_q, dy_q, id_q, c_q):
        dest, filled = slot_table(id_q, EXPERTS, CAP)
        rows_x, rows_dy, rows_c = gather_rows(x_q, dy_q, c_q, filled, TOP)
        return dest, rows_x.reshape(EXPERTS, CAP, D), rows_dy.reshape(EXPERTS, CAP, D), rows_c.reshape(EXPERTS, CAP)

    def one_expert(item):
        inputs, cot_rows, comb_rows, gate_mat, up_mat, down_mat = item
        state = forward_part(inputs, gate_mat, up_mat, down_mat)
        comb_grad, scaled, gate_d, up_d, row_grad = backward_part(state, cot_rows, comb_rows, gate_mat, up_mat, down_mat)
        gate_part = lax.dot_general(inputs, gate_d, first, preferred_element_type=jnp.float32).astype(jnp.bfloat16)
        up_part = lax.dot_general(inputs, up_d, first, preferred_element_type=jnp.float32).astype(jnp.bfloat16)
        down_part = lax.dot_general(state[4], scaled, first, preferred_element_type=jnp.float32).astype(jnp.bfloat16)
        return row_grad, comb_grad, gate_part, up_part, down_part

    def finish(flat_rows, flat_comb, dest):
        picked = jnp.take(flat_rows, dest, axis=0).reshape(TOK_DEV, TOP, D)
        summed = jnp.sum(picked.astype(jnp.float32), axis=1).astype(jnp.bfloat16)
        return summed, jnp.take(flat_comb, dest, axis=0).reshape(TOK_DEV, TOP)

    def one_replica(carry, inputs):
        x_r, dy_r, id_r, c_r = inputs
        dest, rx, rdy, rc = jax.vmap(prepare)(x_r, dy_r, id_r, c_r)
        group_x = jnp.transpose(rx, (1, 0, 2, 3)).reshape(EXPERTS, N_EXPERT * CAP, D)
        group_dy = jnp.transpose(rdy, (1, 0, 2, 3)).reshape(EXPERTS, N_EXPERT * CAP, D)
        group_c = jnp.transpose(rc, (1, 0, 2)).reshape(EXPERTS, N_EXPERT * CAP)
        rows, combs, gate_part, up_part, down_part = lax.map(one_expert, (group_x, group_dy, group_c, w_gate, w_up, w_down))
        gate_part, up_part, down_part = lax.optimization_barrier((gate_part, up_part, down_part))
        carry = (carry[0] + gate_part.astype(jnp.float32), carry[1] + up_part.astype(jnp.float32), carry[2] + down_part.astype(jnp.float32))
        back = jnp.transpose(rows.reshape(EXPERTS, N_EXPERT, CAP, D), (1, 0, 2, 3)).reshape(N_EXPERT, EXPERTS * CAP, D)
        back_c = jnp.transpose(combs.reshape(EXPERTS, N_EXPERT, CAP), (1, 0, 2)).reshape(N_EXPERT, EXPERTS * CAP)
        grads_in, grads_c = jax.vmap(finish)(back, back_c, dest)
        return carry, (grads_in, grads_c)

    start = (jnp.zeros((EXPERTS, D, FF), jnp.float32), jnp.zeros((EXPERTS, D, FF), jnp.float32), jnp.zeros((EXPERTS, FF, D), jnp.float32))
    sums, (grads_in, grads_c) = lax.scan(one_replica, start, (x_all, dy_all, id_all, c_all))
    input_grad = grads_in.reshape(TOKENS, D)
    combine_grad = grads_c.reshape(TOKENS, TOP)
    return (input_grad, combine_grad, sums[0].astype(jnp.bfloat16), sums[1].astype(jnp.bfloat16), sums[2].astype(jnp.bfloat16))
```

```python
import functools
import jax
import jax.numpy as jnp
from jax import lax
from jax.experimental import pallas as pl
from jax.experimental.pallas import tpu as pltpu
from jax.sharding import PartitionSpec as P

MESH = pl.DeviceIdType.MESH
VMEM = pl.BlockSpec(memory_space=pltpu.VMEM)
HBM = pl.BlockSpec(memory_space=pltpu.HBM)
LIMIT = 60 * 1024 * 1024
TILE = 256
PIECES = 4
LAST = (((1,), (1,)), ((), ()))
F32 = jnp.float32
BF16 = jnp.bfloat16


def remote(src, dst, send, recv, axis, target):
    return pltpu.make_async_remote_copy(
        src_ref=src,
        dst_ref=dst,
        send_sem=send,
        recv_sem=recv,
        device_id={axis: target},
        device_id_type=MESH,
    )


def span(index, size):
    return pl.ds(pl.multiple_of(index * size, size), size)


def loop(low, high, body, **options):
    def step(i, carry):
        body(i)
        return carry

    lax.fori_loop(low, high, step, 0, **options)


def layer_kernel(n, bits, *refs):
    ids, comb, x_in, dy_in, g_in, u_in, d_in = refs[:7]
    in_grad, comb_grad, both_out, down_out = refs[7:11]
    x_all, dy_all, x_t, wg, wu, wd, slope, act_all = refs[11:19]
    h_all, h_t, pair_d, hid, rows_out, rows_got = refs[19:25]
    tables, comb_out, comb_got = refs[25:28]
    both_part, down_part = refs[28:30]
    both_got, down_got = refs[30 : 30 + bits], refs[30 + bits : 30 + 2 * bits]
    rest = refs[30 + 2 * bits :]
    load, a_send, a_recv, t_send, t_recv, r_send, r_recv, c_send, c_recv = rest[:9]
    b_send, b_recv, d_send, d_recv = rest[9:13]

    me = lax.axis_index("expert")
    rank = lax.axis_index("dp")
    replicas = 1 << bits
    half = replicas // 2
    rows = in_grad.shape[0]
    feature, width = wg.shape
    piece = feature // PIECES
    chunks = 2 * width // TILE
    both_rows, down_rows = both_out.shape[0], down_out.shape[0]
    bit = [lax.rem(rank // (1 << b), 2) for b in range(bits)]
    mate = [rank + (1 - 2 * bit[b]) * (1 << b) for b in range(bits)]
    orders = ([0] + list(range(1, bits)), [0] + list(range(bits - 1, 0, -1)))
    is_end = jnp.logical_or(me == 0, me == n - 1)
    is_mid = jnp.logical_not(is_end)

    loads = [
        pltpu.make_async_copy(src, dst, load.at[i])
        for i, (src, dst) in enumerate(
            (
                (x_in, x_all.at[span(me, rows)]),
                (dy_in, dy_all.at[span(me, rows)]),
                (g_in.at[0], wg),
                (u_in.at[0], wu),
                (d_in.at[0], wd),
            )
        )
    ]
    for item in loads:
        item.start()
    barrier = pltpu.get_barrier_semaphore()
    for k in range(1, n):
        pl.semaphore_signal(
            barrier, inc=1, device_id={"expert": lax.rem(me + k, n)}, device_id_type=MESH
        )
    for b in range(bits):
        pl.semaphore_signal(barrier, inc=1, device_id={"dp": mate[b]}, device_id_type=MESH)

    lane = lax.broadcasted_iota(jnp.int32, (rows, 128), 1)
    weight = jnp.where(lane == ids[:, 0:1], comb[:, 0:1], 0.0)
    for k in range(1, ids.shape[1]):
        weight = weight + jnp.where(lane == ids[:, k : k + 1], comb[:, k : k + 1], 0.0)
    tables[me] = weight.T[: tables.shape[1]]

    def view(p, block):
        if p is None:
            return x_all.at[span(block, rows)]
        return dy_all.at[span(block, rows), span(p, piece)]

    def index(p):
        return 0 if p is None else 1 + p

    def hop(p, side, s):
        step = 1 - 2 * side
        slot = view(p, jnp.clip(me - step * s, 0, n - 1))
        target = jnp.clip(me + step, 0, n - 1)
        i = index(p)
        return remote(slot, slot, a_send.at[i, side, s], a_recv.at[i, side, s], "expert", target)

    def arrival(p, side, s):
        step = 1 - 2 * side
        slot = view(p, jnp.clip(me - step * (s + 1), 0, n - 1))
        i = index(p)
        return remote(slot, slot, a_send.at[i, side, s], a_recv.at[i, side, s], "expert", me)

    def sends(side, s):
        if side == 0:
            return jnp.logical_and(me >= s, me + 1 < n)
        return jnp.logical_and(me + s < n, me >= 1)

    def passes(side):
        return jnp.where(side == 0, me + 1 < n, me >= 1)

    def table_copy(target):
        return remote(
            tables.at[me], tables.at[me], t_send.at[target], t_recv.at[me], "expert", target
        )

    def row_copy(target):
        return remote(
            rows_out.at[target],
            rows_got.at[me],
            r_send.at[target],
            r_recv.at[me],
            "expert",
            target,
        )

    def comb_copy(target):
        return remote(
            comb_out.at[target],
            comb_got.at[me],
            c_send.at[target],
            c_recv.at[me],
            "expert",
            target,
        )

    pl.semaphore_wait(barrier, n - 1 + bits)
    others = [lax.rem(me + k, n) for k in range(1, n)]
    for target in others:
        table_copy(target).start()
    loads[0].wait()
    for side in range(2):

        @pl.when(sends(side, 0))
        def _():
            hop(None, side, 0).start()

    loads[1].wait()
    for side in range(2):

        @pl.when(sends(side, 0))
        def _():
            for p in range(PIECES):
                hop(p, side, 0).start()

    for item in loads[2:]:
        item.wait()

    def coefficient(b):
        line = tables[b, pl.ds(me, 1), :]
        return jnp.broadcast_to(line, (128, rows)).T[:, 0:1]

    def forward(b):
        own = span(b, rows)
        coef = coefficient(b)

        def tile(j):
            cols = span(j, TILE)
            value = x_all[own, :]
            gate = jnp.dot(value, wg[:, cols], preferred_element_type=F32)
            up = jnp.dot(value, wu[:, cols], preferred_element_type=F32)
            sig = jax.nn.sigmoid(gate)
            act = gate * sig
            hidden = (act * up).astype(BF16)
            slope[own, cols] = up * (sig * (1.0 + gate * (1.0 - sig)))
            act_all[own, cols] = act
            h_all[own, cols] = hidden
            h_t[cols, own] = (coef * hidden.astype(F32)).T.astype(BF16)

        loop(0, width // TILE, tile)

        def turn(j):
            cols = span(j, TILE)
            x_t[cols, own] = x_all[own, cols].T

        loop(0, feature // TILE, turn)

    def gather_hidden(b, q):
        cols = span(q, piece)
        hid[...] += lax.dot_general(
            dy_all[span(b, rows), cols], wd[:, cols], LAST, preferred_element_type=F32
        )

    def slopes(b):
        own = span(b, rows)
        coef = coefficient(b)

        def tile(j, total):
            cols = span(j, TILE)
            grad = hid[:, cols]
            total = total + jnp.sum(h_all[own, cols].astype(F32) * grad, axis=1, keepdims=True)
            grad = coef * grad
            pair_d[own, cols] = (grad * slope[own, cols]).astype(BF16)
            pair_d[own, span(width // TILE + j, TILE)] = (grad * act_all[own, cols]).astype(BF16)
            return total

        total = lax.fori_loop(0, width // TILE, tile, jnp.zeros((rows, 1), F32))
        comb_out[b] = jnp.broadcast_to(total, (rows, 128)).T[:8]

    def input_rows(b):
        own = span(b, rows)

        def tile(j):
            cols = span(j, TILE)
            value = lax.dot_general(
                pair_d[own, :width], wg[cols, :], LAST, preferred_element_type=F32
            )
            value = value + lax.dot_general(
                pair_d[own, width:], wu[cols, :], LAST, preferred_element_type=F32
            )
            rows_out[b, :, cols] = value.astype(BF16)

        loop(0, feature // TILE, tile)

    def send_rows(b):
        row_copy(b).start()
        comb_copy(b).start()

    def distance(d):
        low = jnp.where(jnp.logical_or(d == 0, me >= d), 0, 1)
        high = jnp.where(jnp.logical_and(d > 0, me + d < n), 2, 1)

        def source(side):
            return jnp.clip(me + d * (2 * side - 1), 0, n - 1)

        def take(side):
            @pl.when(d > 0)
            def _():
                arrival(None, side, d - 1).wait_recv()
                b = source(side)
                remote(
                    tables.at[b], tables.at[b], t_send.at[b], t_recv.at[b], "expert", me
                ).wait_recv()

                @pl.when(passes(side))
                def _():
                    hop(None, side, d).start()

        loop(low, high, take)
        loop(low, high, lambda side: forward(source(side)))

        def back(side):
            b = source(side)
            hid[...] = jnp.zeros_like(hid)

            def part(q):
                @pl.when(d > 0)
                def _():
                    arrival(q, side, d - 1).wait_recv()

                    @pl.when(passes(side))
                    def _():
                        hop(q, side, d).start()

                gather_hidden(b, q)

            loop(0, PIECES, part)
            slopes(b)
            input_rows(b)

            @pl.when(jnp.logical_and(is_end, d > 0))
            def _():
                send_rows(b)

        @pl.when(d < n - 1)
        def _():
            loop(low, high, back)

    loop(0, n, distance)

    for target in others:
        inner = jnp.logical_and(target > 0, target < n - 1)

        @pl.when(jnp.logical_and(is_mid, inner))
        def _():
            send_rows(target)

    def rank_of(way, place):
        value = 0
        for i, b in enumerate(orders[way]):
            value = value + lax.rem(place // (1 << (bits - 1 - i)), 2) * (1 << b)
        return value

    def place_of(way, who):
        value = 0
        for i, b in enumerate(orders[way]):
            value = value + lax.rem(who // (1 << b), 2) * (1 << (bits - 1 - i))
        return value

    kinds = {
        "both": (both_part, both_got, b_send, b_recv),
        "down": (down_part, down_got, d_send, d_recv),
    }

    def base(way, i):
        value = 0
        for j in range(i):
            value = value + bit[orders[way][j]] * (replicas >> (j + 1))
        return value

    def stage(kind, c, way, i):
        part, got, send, recv = kinds[kind]
        b = orders[way][i]
        count = replicas >> (i + 1)
        start = base(way, i) + (1 - bit[b]) * count
        return remote(
            part.at[c, pl.ds(start, count)],
            got[i].at[c],
            send.at[c, i],
            recv.at[c, i],
            "dp",
            mate[b],
        )

    def combine(kind, c, way, i):
        part, got, _, _ = kinds[kind]
        count = replicas >> (i + 1)
        start = base(way, i + 1)
        stage(kind, c, way, i).wait_recv()
        if i == bits - 1:
            total = part[c, start].astype(F32) + got[i][c, 0].astype(F32)
            if kind == "both":
                both_out[:, span(c, TILE)] = total.astype(BF16)
            else:
                down_out[:, span(c, piece)] = total.astype(BF16)
            return

        def add(k):
            total = part[c, start + k].astype(F32) + got[i][c, k].astype(F32)
            part[c, start + k] = total.astype(BF16)

        loop(0, count, add)
        stage(kind, c, way, i + 1).start()

    def both_chunk(c, way):
        def place(j):
            where = lax.rem(j + (1 - bit[0]) * half, replicas)
            lines = span(rank_of(way, where), both_rows)
            value = jnp.dot(x_t[lines, :], pair_d[:, span(c, TILE)], preferred_element_type=F32)
            both_part[c, where] = value.astype(BF16)

        loop(0, half, place, unroll=2)
        stage("both", c, way, 0).start()
        loop(half, replicas, place, unroll=2)

    def down_chunk(q, way):
        cols = span(q, piece)
        if down_rows % 16 == 0:

            def place(j):
                where = lax.rem(j + (1 - bit[0]) * half, replicas)
                lines = span(rank_of(way, where), down_rows)
                value = jnp.dot(h_t[lines, :], dy_all[:, cols], preferred_element_type=F32)
                down_part[q, where] = value.astype(BF16)

            loop(0, half, place, unroll=2)
            stage("down", q, way, 0).start()
            loop(half, replicas, place, unroll=2)
        else:

            def place(j):
                lines = span(j, 2 * down_rows)
                value = jnp.dot(h_t[lines, :], dy_all[:, cols], preferred_element_type=F32)
                for k in range(2):
                    some = value[k * down_rows : (k + 1) * down_rows]
                    down_part[q, place_of(way, 2 * j + k)] = some.astype(BF16)

            loop(0, half, place)
            stage("down", q, way, 0).start()

    last = jnp.clip(n - 1 - me, 0, n - 1)
    last_side = jnp.where(me == n - 1, 0, 1)

    @pl.when(is_end)
    def _():
        hid[...] = jnp.zeros_like(hid)

    def early(k):
        for way in range(2):
            q = 2 * k + way

            @pl.when(is_end)
            def _():
                arrival(q, last_side, n - 2).wait_recv()
                gather_hidden(last, q)

            down_chunk(q, way)
            if way == 1:
                combine("down", q - 1, 0, 0)
            else:

                @pl.when(k > 0)
                def _():
                    combine("down", q - 1, 1, 0)

    loop(0, PIECES // 2, early)

    @pl.when(is_end)
    def _():
        slopes(last)

    combine("down", PIECES - 1, 1, 0)

    def late(k):
        for way in range(2):
            c = 2 * k + way
            both_chunk(c, way)
            if way == 1:
                combine("both", c - 1, 0, 0)
            else:

                @pl.when(k > 0)
                def _():
                    combine("both", c - 1, 1, 0)

            @pl.when(jnp.logical_and(k > 0, k <= PIECES // 2))
            def _():
                combine("down", c - 2, way, 1)

    loop(0, chunks // 2, late)
    combine("both", chunks - 1, 1, 0)
    for q in range(max(0, chunks - 2), PIECES):
        combine("down", q, q % 2, 1)

    for side in range(2):
        for s in range(n - 1):

            @pl.when(sends(side, s))
            def _():
                hop(None, side, s).wait_send()
                for p in range(PIECES):
                    hop(p, side, s).wait_send()

    for target in others:
        outer = jnp.logical_or(target == 0, target == n - 1)

        @pl.when(jnp.logical_and(is_mid, outer))
        def _():
            send_rows(target)

    @pl.when(is_end)
    def _():
        input_rows(last)
        send_rows(last)

    for i in range(1, bits):
        for way in range(2):
            if i > 1:
                loop(0, PIECES // 2, lambda k: combine("down", 2 * k + way, way, i))
        if i < bits:

            def step(k):
                for way in range(2):
                    combine("both", 2 * k + way, way, i)

            loop(0, chunks // 2, step)

    for b in others:
        remote(
            rows_got.at[b], rows_got.at[b], r_send.at[b], r_recv.at[b], "expert", me
        ).wait_recv()
        remote(
            comb_got.at[b], comb_got.at[b], c_send.at[b], c_recv.at[b], "expert", me
        ).wait_recv()

    def total_rows(j):
        cols = span(j, TILE)
        total = rows_out[me, :, cols].astype(F32)
        for b in others:
            total = total + rows_got[b, :, cols].astype(F32)
        in_grad[:, cols] = total.astype(BF16)

    loop(0, feature // TILE, total_rows)

    def spread(line):
        return jnp.broadcast_to(line, (128, rows)).T[:, 0:1]

    picked = jnp.where(ids[...] == me, spread(comb_out[me, 0:1, :]), 0.0)
    for b in others:
        picked = picked + jnp.where(ids[...] == b, spread(comb_got[b, 0:1, :]), 0.0)
    comb_grad[...] = picked

    for target in others:
        table_copy(target).wait_send()
        row_copy(target).wait_send()
        comb_copy(target).wait_send()
    for kind, count in (("both", chunks), ("down", PIECES)):

        def drain(k):
            for way in range(2):
                for i in range(bits):
                    stage(kind, 2 * k + way, way, i).wait_send()

        loop(0, count // 2, drain)


def shards(tokens, cotangent, expert_ids, combine, w_gate, w_up, w_down):
    n = lax.axis_size("expert")
    replicas = lax.axis_size("dp")
    bits = replicas.bit_length() - 1
    rows, top = expert_ids.shape
    feature = tokens.shape[1]
    width = w_gate.shape[2]
    everyone = n * rows
    chunks = 2 * width // TILE
    piece = feature // PIECES
    both_rows, down_rows = feature // replicas, width // replicas
    table = -(-n // 8) * 8
    outs = [
        jax.ShapeDtypeStruct((rows, feature), BF16),
        jax.ShapeDtypeStruct((rows, top), F32),
        jax.ShapeDtypeStruct((both_rows, 2 * width), BF16),
        jax.ShapeDtypeStruct((down_rows, feature), BF16),
    ]
    scratch = [
        pltpu.VMEM((everyone, feature), BF16),
        pltpu.VMEM((everyone, feature), BF16),
        pltpu.VMEM((feature, everyone), BF16),
        pltpu.VMEM((feature, width), BF16),
        pltpu.VMEM((feature, width), BF16),
        pltpu.VMEM((width, feature), BF16),
        pltpu.VMEM((everyone, width), F32),
        pltpu.VMEM((everyone, width), F32),
        pltpu.VMEM((everyone, width), BF16),
        pltpu.VMEM((width, everyone), BF16),
        pltpu.VMEM((everyone, 2 * width), BF16),
        pltpu.VMEM((rows, width), F32),
        pltpu.VMEM((n, rows, feature), BF16),
        pltpu.VMEM((n, rows, feature), BF16),
        pltpu.VMEM((n, table, rows), F32),
        pltpu.VMEM((n, 8, rows), F32),
        pltpu.VMEM((n, 8, rows), F32),
        pltpu.VMEM((chunks, replicas, both_rows, TILE), BF16),
        pltpu.VMEM((PIECES, replicas, down_rows, piece), BF16),
    ]
    for i in range(bits):
        scratch.append(pltpu.VMEM((chunks, replicas >> (i + 1), both_rows, TILE), BF16))
    for i in range(bits):
        scratch.append(pltpu.VMEM((PIECES, replicas >> (i + 1), down_rows, piece), BF16))
    scratch += [pltpu.SemaphoreType.DMA((5,))]
    scratch += [pltpu.SemaphoreType.DMA((1 + PIECES, 2, n))] * 2
    scratch += [pltpu.SemaphoreType.DMA((n,))] * 6
    scratch += [pltpu.SemaphoreType.DMA((chunks, bits))] * 2
    scratch += [pltpu.SemaphoreType.DMA((PIECES, bits))] * 2
    input_grad, combine_grad, both, down = pl.pallas_call(
        functools.partial(layer_kernel, n, bits),
        out_shape=outs,
        in_specs=[VMEM] * 2 + [HBM] * 5,
        out_specs=[VMEM] * 4,
        scratch_shapes=scratch,
        compiler_params=pltpu.CompilerParams(
            collective_id=0, has_side_effects=True, vmem_limit_bytes=LIMIT
        ),
        name="layer",
    )(expert_ids, combine, tokens, cotangent, w_gate, w_up, w_down)
    return (input_grad, combine_grad, both[None, :, :width], both[None, :, width:], down[None])


def solution(mesh):
    by_token = P(("dp", "expert"), None)
    by_expert = P("expert", None, None)
    by_row = P("expert", "dp", None)
    return jax.shard_map(
        shards,
        mesh=mesh,
        in_specs=(by_token,) * 4 + (by_expert,) * 3,
        out_specs=(by_token, by_token, by_row, by_row, by_row),
        check_vma=False,
    )
```

```python
import functools
import jax
import jax.numpy as jnp
from jax import lax
from jax.experimental import pallas as pl
from jax.experimental.pallas import tpu as pltpu
from jax.sharding import PartitionSpec as P

MESH = pl.DeviceIdType.MESH
VMEM = pl.BlockSpec(memory_space=pltpu.VMEM)
HBM = pl.BlockSpec(memory_space=pltpu.HBM)
LIMIT = 50 * 1024 * 1024
TILE = 256
WIDE = 512
PIECES = 4
LAST = (((1,), (1,)), ((), ()))
F32 = jnp.float32
BF16 = jnp.bfloat16


def remote(src, dst, send, recv, axis, target):
    return pltpu.make_async_remote_copy(
        src_ref=src,
        dst_ref=dst,
        send_sem=send,
        recv_sem=recv,
        device_id={axis: target},
        device_id_type=MESH,
    )


def span(index, size):
    return pl.ds(pl.multiple_of(index * size, size), size)


def loop(low, high, body, **options):
    def step(i, carry):
        body(i)
        return carry

    lax.fori_loop(low, high, step, 0, **options)


def layer_kernel(n, bits, *refs):
    ids, comb, x_in, dy_in, g_in, u_in, d_in = refs[:7]
    in_grad, comb_grad, both_out, down_out = refs[7:11]
    x_all, dy_all, x_t, wg, wu, wd, slope, act_all = refs[11:19]
    h_all, h_t, pair_d, hid, rows_out, rows_got = refs[19:25]
    tables, comb_out, comb_got = refs[25:28]
    both_part, down_part = refs[28:30]
    both_got, down_got = refs[30 : 30 + bits], refs[30 + bits : 30 + 2 * bits]
    rest = refs[30 + 2 * bits :]
    load, a_send, a_recv, t_send, t_recv, r_send, r_recv, c_send, c_recv = rest[:9]
    b_send, b_recv, d_send, d_recv, f_send, f_recv = rest[9:15]

    me = lax.axis_index("expert")
    rank = lax.axis_index("dp")
    replicas = 1 << bits
    half = replicas // 2
    rows = in_grad.shape[0]
    feature, width = wg.shape
    piece = feature // PIECES
    chunks = 2 * width // TILE
    both_rows, down_rows = both_out.shape[0], down_out.shape[0]
    bit = [lax.rem(rank // (1 << b), 2) for b in range(bits)]
    mate = [rank + (1 - 2 * bit[b]) * (1 << b) for b in range(bits)]
    orders = ([0] + list(range(1, bits)), [0] + list(range(bits - 1, 0, -1)))
    is_end = jnp.logical_or(me == 0, me == n - 1)
    is_mid = jnp.logical_not(is_end)

    loads = [
        pltpu.make_async_copy(src, dst, load.at[i])
        for i, (src, dst) in enumerate(
            (
                (g_in.at[0], wg),
                (u_in.at[0], wu),
                (d_in.at[0], wd),
            )
        )
    ]
    for item in loads:
        item.start()
    barrier = pltpu.get_barrier_semaphore()
    for k in range(1, n):
        pl.semaphore_signal(
            barrier, inc=1, device_id={"expert": lax.rem(me + k, n)}, device_id_type=MESH
        )
    for b in range(bits):
        pl.semaphore_signal(barrier, inc=1, device_id={"dp": mate[b]}, device_id_type=MESH)

    expert = lax.broadcasted_iota(jnp.int32, tables.shape[1:], 0)
    weight = jnp.where(expert == ids[0:1, :], comb[0:1, :], 0.0)
    for k in range(1, ids.shape[0]):
        weight = weight + jnp.where(expert == ids[k : k + 1, :], comb[k : k + 1, :], 0.0)
    tables[me] = weight

    def view(p, block):
        if p is None:
            return x_all.at[span(block, rows)]
        return dy_all.at[span(block, rows), span(p, piece)]

    def index(p):
        return 0 if p is None else 1 + p

    def hop(p, side, s, own=False):
        step = 1 - 2 * side
        slot = view(p, jnp.clip(me - step * s, 0, n - 1))
        target = jnp.clip(me + step, 0, n - 1)
        i = index(p)
        src = slot
        if own:
            src = x_in if p is None else dy_in.at[:, span(p, piece)]
        return remote(src, slot, a_send.at[i, side, s], a_recv.at[i, side, s], "expert", target)

    def arrival(p, side, s):
        step = 1 - 2 * side
        slot = view(p, jnp.clip(me - step * (s + 1), 0, n - 1))
        i = index(p)
        return remote(slot, slot, a_send.at[i, side, s], a_recv.at[i, side, s], "expert", me)

    def sends(side, s):
        if side == 0:
            return jnp.logical_and(me >= s, me + 1 < n)
        return jnp.logical_and(me + s < n, me >= 1)

    def passes(side):
        return jnp.where(side == 0, me + 1 < n, me >= 1)

    def table_copy(target):
        return remote(
            tables.at[me], tables.at[me], t_send.at[target], t_recv.at[me], "expert", target
        )

    def row_copy(target):
        return remote(
            rows_out.at[target],
            rows_got.at[me],
            r_send.at[target],
            r_recv.at[me],
            "expert",
            target,
        )

    fold = n == 4
    ally = n - 1 - me
    near = jnp.where(2 * me < n, 0, n - 1)
    far = n - 1 - near

    def fold_copy():
        return remote(
            rows_out.at[far], rows_got.at[ally], f_send.at[0], f_recv.at[0], "expert", ally
        )

    def folded():
        slot = rows_got.at[me]
        return remote(slot, slot, f_send.at[0], f_recv.at[0], "expert", me)

    def comb_copy(target):
        return remote(
            comb_out.at[target],
            comb_got.at[me],
            c_send.at[target],
            c_recv.at[me],
            "expert",
            target,
        )

    pl.semaphore_wait(barrier, n - 1 + bits)
    others = [lax.rem(me + k, n) for k in range(1, n)]
    for target in others:
        table_copy(target).start()
    for p in [None] + list(range(PIECES)):
        for side in range(2):

            @pl.when(sends(side, 0))
            def _():
                hop(p, side, 0, True).start()

    x_all[span(me, rows), :] = x_in[...]
    dy_all[span(me, rows), :] = dy_in[...]
    for item in loads:
        item.wait()

    def coefficient(b):
        line = tables[b, pl.ds(me, 1), :]
        return jnp.broadcast_to(line, (128, rows)).T[:, 0:1]

    def forward(b):
        own = span(b, rows)
        coef = coefficient(b)

        def tile(j):
            cols = span(j, TILE)
            value = x_all[own, :]
            gate = jnp.dot(value, wg[:, cols], preferred_element_type=F32)
            up = jnp.dot(value, wu[:, cols], preferred_element_type=F32)
            sig = jax.nn.sigmoid(gate)
            act = gate * sig
            hidden = (act * up).astype(BF16)
            slope[own, cols] = up * (sig * (1.0 + gate * (1.0 - sig)))
            act_all[own, cols] = act
            h_all[own, cols] = hidden
            h_t[cols, own] = (coef * hidden.astype(F32)).T.astype(BF16)

        loop(0, width // TILE, tile)

        def turn(j):
            cols = span(j, TILE)
            x_t[cols, own] = x_all[own, cols].T

        loop(0, feature // TILE, turn)

    def gather_hidden(b, q):
        cols = span(q, piece)
        hid[...] += lax.dot_general(
            dy_all[span(b, rows), cols], wd[:, cols], LAST, preferred_element_type=F32
        )

    def slopes(b):
        own = span(b, rows)
        coef = coefficient(b)

        def tile(j, total):
            cols = span(j, TILE)
            grad = hid[:, cols]
            total = total + jnp.sum(h_all[own, cols].astype(F32) * grad, axis=1, keepdims=True)
            grad = coef * grad
            pair_d[own, cols] = (grad * slope[own, cols]).astype(BF16)
            pair_d[own, span(width // TILE + j, TILE)] = (grad * act_all[own, cols]).astype(BF16)
            return total

        total = lax.fori_loop(0, width // TILE, tile, jnp.zeros((rows, 1), F32))
        comb_out[b] = jnp.broadcast_to(total, (rows, 128)).T[:8]

    def input_tile(b, j):
        own = span(b, rows)
        cols = span(j, WIDE)
        value = lax.dot_general(pair_d[own, :width], wg[cols, :], LAST, preferred_element_type=F32)
        value = value + lax.dot_general(
            pair_d[own, width:], wu[cols, :], LAST, preferred_element_type=F32
        )
        rows_out[b, :, cols] = value.astype(BF16)

    def send_rows(b):
        row_copy(b).start()
        comb_copy(b).start()

    def distance(d):
        low = jnp.where(jnp.logical_or(d == 0, me >= d), 0, 1)
        high = jnp.where(jnp.logical_and(d > 0, me + d < n), 2, 1)

        def source(side):
            return jnp.clip(me + d * (2 * side - 1), 0, n - 1)

        def take(side):
            @pl.when(d > 0)
            def _():
                arrival(None, side, d - 1).wait_recv()
                b = source(side)
                remote(
                    tables.at[b], tables.at[b], t_send.at[b], t_recv.at[b], "expert", me
                ).wait_recv()

                @pl.when(passes(side))
                def _():
                    hop(None, side, d).start()

        loop(low, high, take)
        loop(low, high, lambda side: forward(source(side)))

        def back(side):
            b = source(side)
            hid[...] = jnp.zeros_like(hid)

            def part(q):
                @pl.when(d > 0)
                def _():
                    arrival(q, side, d - 1).wait_recv()

                    @pl.when(passes(side))
                    def _():
                        hop(q, side, d).start()

                gather_hidden(b, q)

            loop(0, PIECES, part)
            slopes(b)
            loop(0, feature // WIDE, functools.partial(input_tile, b))

            @pl.when(jnp.logical_and(is_end, d > 0))
            def _():
                send_rows(b)

        @pl.when(d < n - 1)
        def _():
            loop(low, high, back)

    loop(0, n, distance)

    if fold:

        @pl.when(is_mid)
        def _():
            fold_copy().start()
            send_rows(ally)

    else:
        for target in others:
            inner = jnp.logical_and(target > 0, target < n - 1)

            @pl.when(jnp.logical_and(is_mid, inner))
            def _():
                send_rows(target)

    def rank_of(way, place):
        value = 0
        for i, b in enumerate(orders[way]):
            value = value + lax.rem(place // (1 << (bits - 1 - i)), 2) * (1 << b)
        return value

    def place_of(way, who):
        value = 0
        for i, b in enumerate(orders[way]):
            value = value + lax.rem(who // (1 << b), 2) * (1 << (bits - 1 - i))
        return value

    kinds = {
        "both": (both_part, both_got, b_send, b_recv),
        "down": (down_part, down_got, d_send, d_recv),
    }

    def base(way, i):
        value = 0
        for j in range(i):
            value = value + bit[orders[way][j]] * (replicas >> (j + 1))
        return value

    def stage(kind, c, way, i):
        part, got, send, recv = kinds[kind]
        b = orders[way][i]
        count = replicas >> (i + 1)
        start = base(way, i) + (1 - bit[b]) * count
        return remote(
            part.at[c, pl.ds(start, count)],
            got[i].at[c],
            send.at[c, i],
            recv.at[c, i],
            "dp",
            mate[b],
        )

    def combine(kind, c, way, i):
        part, got, _, _ = kinds[kind]
        count = replicas >> (i + 1)
        start = base(way, i + 1)
        stage(kind, c, way, i).wait_recv()
        if i == bits - 1:
            total = part[c, start].astype(F32) + got[i][c, 0].astype(F32)
            if kind == "both":
                both_out[:, span(c, TILE)] = total.astype(BF16)
            else:
                down_out[:, span(c, piece)] = total.astype(BF16)
            return

        def add(k):
            total = part[c, start + k].astype(F32) + got[i][c, k].astype(F32)
            part[c, start + k] = total.astype(BF16)

        loop(0, count, add)
        stage(kind, c, way, i + 1).start()

    def both_chunk(c, way):
        def place(j):
            where = lax.rem(j + (1 - bit[0]) * half, replicas)
            lines = span(rank_of(way, where), both_rows)
            value = jnp.dot(x_t[lines, :], pair_d[:, span(c, TILE)], preferred_element_type=F32)
            both_part[c, where] = value.astype(BF16)

        loop(0, half, place, unroll=2)
        stage("both", c, way, 0).start()
        loop(half, replicas, place, unroll=2)

    def down_chunk(q, way):
        cols = span(q, piece)
        if down_rows % 16 == 0:

            def place(j):
                where = lax.rem(j + (1 - bit[0]) * half, replicas)
                lines = span(rank_of(way, where), down_rows)
                value = jnp.dot(h_t[lines, :], dy_all[:, cols], preferred_element_type=F32)
                down_part[q, where] = value.astype(BF16)

            loop(0, half, place, unroll=2)
            stage("down", q, way, 0).start()
            loop(half, replicas, place, unroll=2)
        else:

            def place(j):
                lines = span(j, 2 * down_rows)
                value = jnp.dot(h_t[lines, :], dy_all[:, cols], preferred_element_type=F32)
                for k in range(2):
                    some = value[k * down_rows : (k + 1) * down_rows]
                    down_part[q, place_of(way, 2 * j + k)] = some.astype(BF16)

            loop(0, half, place)
            stage("down", q, way, 0).start()

    last = jnp.clip(n - 1 - me, 0, n - 1)
    last_side = jnp.where(me == n - 1, 0, 1)

    @pl.when(is_end)
    def _():
        hid[...] = jnp.zeros_like(hid)

    def early(k):
        for way in range(2):
            q = 2 * k + way
            if way == 1:
                combine("down", q - 1, 0, 0)
            else:

                @pl.when(k > 0)
                def _():
                    combine("down", q - 1, 1, 0)

            @pl.when(is_end)
            def _():
                arrival(q, last_side, n - 2).wait_recv()
                gather_hidden(last, q)

            if way == 1:

                @pl.when(jnp.logical_and(is_end, q == PIECES - 1))
                def _():
                    slopes(last)

            down_chunk(q, way)

    loop(0, PIECES // 2, early)
    wide = feature // WIDE
    share = -(-wide // (chunks - 2))

    def late(k):
        for way in range(2):
            c = 2 * k + way
            both_chunk(c, way)
            if way == 1:
                combine("both", c - 1, 0, 0)
            else:

                @pl.when(k == 0)
                def _():
                    combine("down", PIECES - 1, 1, 0)

                @pl.when(k > 0)
                def _():
                    combine("both", c - 1, 1, 0)

            for t in range(share):
                j = share * (c - 2) + t

                @pl.when(jnp.logical_and(is_end, jnp.logical_and(k > 0, j < wide)))
                def _():
                    input_tile(last, j)

            @pl.when(jnp.logical_and(k > 0, k <= PIECES // 2))
            def _():
                combine("down", c - 2, way, 1)

    loop(0, chunks // 2, late)
    combine("both", chunks - 1, 1, 0)
    for q in range(max(0, chunks - 2), PIECES):
        combine("down", q, q % 2, 1)

    @pl.when(is_end)
    def _():
        send_rows(last)

    for side in range(2):
        for s in range(n - 1):

            @pl.when(sends(side, s))
            def _():
                hop(None, side, s).wait_send()
                for p in range(PIECES):
                    hop(p, side, s).wait_send()

    if fold:

        @pl.when(is_mid)
        def _():
            folded().wait_recv()

            def add(j):
                cols = span(j, TILE)
                total = rows_out[near, :, cols].astype(F32) + rows_got[me, :, cols].astype(F32)
                rows_out[near, :, cols] = total.astype(BF16)

            loop(0, feature // TILE, add)
            row_copy(near).start()
            comb_copy(near).start()
            comb_copy(far).start()

    else:
        for target in others:
            outer = jnp.logical_or(target == 0, target == n - 1)

            @pl.when(jnp.logical_and(is_mid, outer))
            def _():
                send_rows(target)

    for i in range(1, bits - 1):
        if i > 1:
            for way in range(2):
                loop(0, PIECES // 2, lambda k: combine("down", 2 * k + way, way, i))

        def step(k):
            for way in range(2):
                combine("both", 2 * k + way, way, i)

        loop(0, chunks // 2, step)

    for way in range(2):
        loop(0, PIECES // 2, lambda k: combine("down", 2 * k + way, way, bits - 1))

    def takes_row(b):
        if not fold:
            return b >= 0
        return jnp.logical_or(is_mid, b != jnp.where(me == 0, n - 2, 1))

    def gives_row(target):
        if not fold:
            return target >= 0
        return jnp.logical_or(is_end, target != far)

    for b in others:

        @pl.when(takes_row(b))
        def _():
            remote(
                rows_got.at[b], rows_got.at[b], r_send.at[b], r_recv.at[b], "expert", me
            ).wait_recv()

        remote(
            comb_got.at[b], comb_got.at[b], c_send.at[b], c_recv.at[b], "expert", me
        ).wait_recv()

    def total_rows(who):
        def tile(j):
            cols = span(j, TILE)
            total = rows_out[me, :, cols].astype(F32)
            for b in who:
                total = total + rows_got[b, :, cols].astype(F32)
            in_grad[:, cols] = total.astype(BF16)

        loop(0, feature // TILE, tile)

    if fold:

        @pl.when(is_end)
        def _():
            total_rows([n - 1 - me, jnp.where(me == 0, 1, n - 2)])

        @pl.when(is_mid)
        def _():
            total_rows(others)

    else:
        total_rows(others)

    picked = jnp.where(ids[...] == me, comb_out[me, 0:1, :], 0.0)
    for b in others:
        picked = picked + jnp.where(ids[...] == b, comb_got[b, 0:1, :], 0.0)
    comb_grad[...] = picked

    def finish(k):
        for way in range(2):
            combine("both", 2 * k + way, way, bits - 1)

    loop(0, chunks // 2, finish)

    for target in others:
        table_copy(target).wait_send()
        comb_copy(target).wait_send()

        @pl.when(gives_row(target))
        def _():
            row_copy(target).wait_send()

    if fold:

        @pl.when(is_mid)
        def _():
            fold_copy().wait_send()

    for kind, count in (("both", chunks), ("down", PIECES)):

        def drain(k):
            for way in range(2):
                for i in range(bits):
                    stage(kind, 2 * k + way, way, i).wait_send()

        loop(0, count // 2, drain)


def deliver_kernel(rows, comb, both, down, *refs):
    outs, sems = refs[:-1], refs[-1]
    width = outs[2].shape[2]
    copies = []
    for src, dst in (
        (rows, outs[0]),
        (both.at[:, pl.ds(0, width)], outs[2].at[0]),
        (both.at[:, pl.ds(width, width)], outs[3].at[0]),
        (down, outs[4].at[0]),
        (comb, outs[1]),
    ):
        copies.append(pltpu.make_async_copy(src, dst, sems.at[len(copies)]))
        copies[-1].start()
    for copy in copies:
        copy.wait()


def deliver(rows, comb, both, down):
    width = both.shape[1] // 2
    outs = [
        jax.ShapeDtypeStruct(rows.shape, BF16),
        jax.ShapeDtypeStruct(comb.shape, F32),
        jax.ShapeDtypeStruct((1, both.shape[0], width), BF16),
        jax.ShapeDtypeStruct((1, both.shape[0], width), BF16),
        jax.ShapeDtypeStruct((1,) + down.shape, BF16),
    ]
    input_grad, combine_grad, gate_grad, up_grad, down_grad = pl.pallas_call(
        deliver_kernel,
        out_shape=outs,
        in_specs=[VMEM] * 4,
        out_specs=[HBM] * 5,
        scratch_shapes=[pltpu.SemaphoreType.DMA((5,))],
        compiler_params=pltpu.CompilerParams(vmem_limit_bytes=8 * 1024 * 1024),
        name="deliver",
    )(rows, comb, both, down)
    return (input_grad, combine_grad.T, gate_grad, up_grad, down_grad)


def shards(tokens, cotangent, expert_ids, combine, w_gate, w_up, w_down):
    n = lax.axis_size("expert")
    replicas = lax.axis_size("dp")
    bits = replicas.bit_length() - 1
    rows, top = expert_ids.shape
    feature = tokens.shape[1]
    width = w_gate.shape[2]
    everyone = n * rows
    chunks = 2 * width // TILE
    piece = feature // PIECES
    both_rows, down_rows = feature // replicas, width // replicas
    table = -(-n // 8) * 8
    outs = [
        jax.ShapeDtypeStruct((rows, feature), BF16),
        jax.ShapeDtypeStruct((top, rows), F32),
        jax.ShapeDtypeStruct((both_rows, 2 * width), BF16),
        jax.ShapeDtypeStruct((down_rows, feature), BF16),
    ]
    scratch = [
        pltpu.VMEM((everyone, feature), BF16),
        pltpu.VMEM((everyone, feature), BF16),
        pltpu.VMEM((feature, everyone), BF16),
        pltpu.VMEM((feature, width), BF16),
        pltpu.VMEM((feature, width), BF16),
        pltpu.VMEM((width, feature), BF16),
        pltpu.VMEM((everyone, width), F32),
        pltpu.VMEM((everyone, width), F32),
        pltpu.VMEM((everyone, width), BF16),
        pltpu.VMEM((width, everyone), BF16),
        pltpu.VMEM((everyone, 2 * width), BF16),
        pltpu.VMEM((rows, width), F32),
        pltpu.VMEM((n, rows, feature), BF16),
        pltpu.VMEM((n, rows, feature), BF16),
        pltpu.VMEM((n, table, rows), F32),
        pltpu.VMEM((n, 8, rows), F32),
        pltpu.VMEM((n, 8, rows), F32),
        pltpu.VMEM((chunks, replicas, both_rows, TILE), BF16),
        pltpu.VMEM((PIECES, replicas, down_rows, piece), BF16),
    ]
    for i in range(bits):
        scratch.append(pltpu.VMEM((chunks, replicas >> (i + 1), both_rows, TILE), BF16))
    for i in range(bits):
        scratch.append(pltpu.VMEM((PIECES, replicas >> (i + 1), down_rows, piece), BF16))
    scratch += [pltpu.SemaphoreType.DMA((3,))]
    scratch += [pltpu.SemaphoreType.DMA((1 + PIECES, 2, n))] * 2
    scratch += [pltpu.SemaphoreType.DMA((n,))] * 6
    scratch += [pltpu.SemaphoreType.DMA((chunks, bits))] * 2
    scratch += [pltpu.SemaphoreType.DMA((PIECES, bits))] * 2
    scratch += [pltpu.SemaphoreType.DMA((1,))] * 2
    input_grad, combine_grad, both, down = pl.pallas_call(
        functools.partial(layer_kernel, n, bits),
        out_shape=outs,
        in_specs=[VMEM] * 4 + [HBM] * 3,
        out_specs=[VMEM] * 4,
        scratch_shapes=scratch,
        compiler_params=pltpu.CompilerParams(
            collective_id=0, has_side_effects=True, vmem_limit_bytes=LIMIT
        ),
        name="layer",
    )(expert_ids.T, combine.T, tokens, cotangent, w_gate, w_up, w_down)
    return deliver(input_grad, combine_grad, both, down)


def solution(mesh):
    by_token = P(("dp", "expert"), None)
    by_expert = P("expert", None, None)
    by_row = P("expert", "dp", None)
    return jax.shard_map(
        shards,
        mesh=mesh,
        in_specs=(by_token,) * 4 + (by_expert,) * 3,
        out_specs=(by_token, by_token, by_row, by_row, by_row),
        check_vma=False,
    )
```

```python
import functools
import jax
import jax.numpy as jnp
from jax import lax
from jax.experimental import pallas as pl
from jax.experimental.pallas import tpu as pltpu
from jax.sharding import PartitionSpec as P

MESH = pl.DeviceIdType.MESH
VMEM = pl.BlockSpec(memory_space=pltpu.VMEM)
HBM = pl.BlockSpec(memory_space=pltpu.HBM)
LIMIT = 50 * 1024 * 1024
TILE = 256
WIDE = 512
PIECES = 4
LAST = (((1,), (1,)), ((), ()))
F32 = jnp.float32
BF16 = jnp.bfloat16


def remote(src, dst, send, recv, axis, target):
    return pltpu.make_async_remote_copy(
        src_ref=src,
        dst_ref=dst,
        send_sem=send,
        recv_sem=recv,
        device_id={axis: target},
        device_id_type=MESH,
    )


def span(index, size):
    return pl.ds(pl.multiple_of(index * size, size), size)


def loop(low, high, body, **options):
    def step(i, carry):
        body(i)
        return carry

    lax.fori_loop(low, high, step, 0, **options)


def layer_kernel(n, bits, *refs):
    ids, comb, x_in, dy_in, g_in, u_in, d_in = refs[:7]
    in_grad, comb_grad, both_out, down_out = refs[7:11]
    x_all, dy_all, x_t, wg, wu, wd, slope, act_all = refs[11:19]
    h_all, h_t, pair_d, hid, rows_out, rows_got = refs[19:25]
    tables, comb_out, comb_got = refs[25:28]
    both_part, down_part = refs[28:30]
    both_got, down_got = refs[30 : 30 + bits], refs[30 + bits : 30 + 2 * bits]
    rest = refs[30 + 2 * bits :]
    load, a_send, a_recv, t_send, t_recv, r_send, r_recv, c_send, c_recv = rest[:9]
    b_send, b_recv, d_send, d_recv, f_send, f_recv = rest[9:15]

    me = lax.axis_index("expert")
    rank = lax.axis_index("dp")
    replicas = 1 << bits
    half = replicas // 2
    rows = in_grad.shape[0]
    feature, width = wg.shape
    piece = feature // PIECES
    chunks = 2 * width // TILE
    both_rows, down_rows = both_out.shape[0], down_out.shape[0]
    bit = [lax.rem(rank // (1 << b), 2) for b in range(bits)]
    mate = [rank + (1 - 2 * bit[b]) * (1 << b) for b in range(bits)]
    orders = ([0] + list(range(1, bits)), [0] + list(range(bits - 1, 0, -1)))
    is_end = jnp.logical_or(me == 0, me == n - 1)
    is_mid = jnp.logical_not(is_end)

    loads = [
        pltpu.make_async_copy(src, dst, load.at[i])
        for i, (src, dst) in enumerate(
            (
                (g_in.at[0], wg),
                (u_in.at[0], wu),
                (d_in.at[0], wd),
            )
        )
    ]
    for item in loads:
        item.start()
    barrier = pltpu.get_barrier_semaphore()
    for k in range(1, n):
        pl.semaphore_signal(
            barrier, inc=1, device_id={"expert": lax.rem(me + k, n)}, device_id_type=MESH
        )
    for b in range(bits):
        pl.semaphore_signal(barrier, inc=1, device_id={"dp": mate[b]}, device_id_type=MESH)

    expert = lax.broadcasted_iota(jnp.int32, tables.shape[1:], 0)
    weight = jnp.where(expert == ids[0:1, :], comb[0:1, :], 0.0)
    for k in range(1, ids.shape[0]):
        weight = weight + jnp.where(expert == ids[k : k + 1, :], comb[k : k + 1, :], 0.0)
    tables[me] = weight

    def view(p, block):
        if p is None:
            return x_all.at[span(block, rows)]
        return dy_all.at[span(block, rows), span(p, piece)]

    def index(p):
        return 0 if p is None else 1 + p

    def hop(p, side, s, own=False):
        step = 1 - 2 * side
        slot = view(p, jnp.clip(me - step * s, 0, n - 1))
        target = jnp.clip(me + step, 0, n - 1)
        i = index(p)
        src = slot
        if own:
            src = x_in if p is None else dy_in.at[:, span(p, piece)]
        return remote(src, slot, a_send.at[i, side, s], a_recv.at[i, side, s], "expert", target)

    def arrival(p, side, s):
        step = 1 - 2 * side
        slot = view(p, jnp.clip(me - step * (s + 1), 0, n - 1))
        i = index(p)
        return remote(slot, slot, a_send.at[i, side, s], a_recv.at[i, side, s], "expert", me)

    def sends(side, s):
        if side == 0:
            return jnp.logical_and(me >= s, me + 1 < n)
        return jnp.logical_and(me + s < n, me >= 1)

    def passes(side):
        return jnp.where(side == 0, me + 1 < n, me >= 1)

    def table_copy(target):
        return remote(
            tables.at[me], tables.at[me], t_send.at[target], t_recv.at[me], "expert", target
        )

    def row_copy(target):
        return remote(
            rows_out.at[target],
            rows_got.at[me],
            r_send.at[target],
            r_recv.at[me],
            "expert",
            target,
        )

    fold = n == 4
    ally = n - 1 - me
    near = jnp.where(2 * me < n, 0, n - 1)
    far = n - 1 - near

    def fold_copy():
        return remote(
            rows_out.at[far], rows_got.at[ally], f_send.at[0], f_recv.at[0], "expert", ally
        )

    def folded():
        slot = rows_got.at[me]
        return remote(slot, slot, f_send.at[0], f_recv.at[0], "expert", me)

    def comb_copy(target):
        return remote(
            comb_out.at[target],
            comb_got.at[me],
            c_send.at[target],
            c_recv.at[me],
            "expert",
            target,
        )

    pl.semaphore_wait(barrier, n - 1 + bits)
    others = [lax.rem(me + k, n) for k in range(1, n)]
    for target in others:
        table_copy(target).start()
    for p in [None] + list(range(PIECES)):
        for side in range(2):

            @pl.when(sends(side, 0))
            def _():
                hop(p, side, 0, True).start()

    x_all[span(me, rows), :] = x_in[...]
    dy_all[span(me, rows), :] = dy_in[...]
    for item in loads:
        item.wait()

    def coefficient(b):
        line = tables[b, pl.ds(me, 1), :]
        return jnp.broadcast_to(line, (128, rows)).T[:, 0:1]

    def forward(b):
        own = span(b, rows)
        coef = coefficient(b)

        def tile(j):
            cols = span(j, TILE)
            value = x_all[own, :]
            gate = jnp.dot(value, wg[:, cols], preferred_element_type=F32)
            up = jnp.dot(value, wu[:, cols], preferred_element_type=F32)
            sig = jax.nn.sigmoid(gate)
            act = gate * sig
            hidden = (act * up).astype(BF16)
            slope[own, cols] = up * (sig * (1.0 + gate * (1.0 - sig)))
            act_all[own, cols] = act
            h_all[own, cols] = hidden
            h_t[cols, own] = (coef * hidden.astype(F32)).T.astype(BF16)

        loop(0, width // TILE, tile)

        def turn(j):
            cols = span(j, TILE)
            x_t[cols, own] = x_all[own, cols].T

        loop(0, feature // TILE, turn)

    def gather_hidden(b, q):
        cols = span(q, piece)
        hid[...] += lax.dot_general(
            dy_all[span(b, rows), cols], wd[:, cols], LAST, preferred_element_type=F32
        )

    def slopes(b):
        own = span(b, rows)
        coef = coefficient(b)

        def tile(j, total):
            cols = span(j, TILE)
            grad = hid[:, cols]
            total = total + jnp.sum(h_all[own, cols].astype(F32) * grad, axis=1, keepdims=True)
            grad = coef * grad
            pair_d[own, cols] = (grad * slope[own, cols]).astype(BF16)
            pair_d[own, span(width // TILE + j, TILE)] = (grad * act_all[own, cols]).astype(BF16)
            return total

        total = lax.fori_loop(0, width // TILE, tile, jnp.zeros((rows, 1), F32))
        comb_out[b] = jnp.broadcast_to(total, (rows, 128)).T[:8]

    def input_tile(b, j):
        own = span(b, rows)
        cols = span(j, WIDE)
        value = lax.dot_general(pair_d[own, :width], wg[cols, :], LAST, preferred_element_type=F32)
        value = value + lax.dot_general(
            pair_d[own, width:], wu[cols, :], LAST, preferred_element_type=F32
        )
        rows_out[b, :, cols] = value.astype(BF16)

    def send_rows(b):
        row_copy(b).start()
        comb_copy(b).start()

    def distance(d):
        low = jnp.where(jnp.logical_or(d == 0, me >= d), 0, 1)
        high = jnp.where(jnp.logical_and(d > 0, me + d < n), 2, 1)

        def source(side):
            return jnp.clip(me + d * (2 * side - 1), 0, n - 1)

        def take(side):
            @pl.when(d > 0)
            def _():
                arrival(None, side, d - 1).wait_recv()
                b = source(side)
                remote(
                    tables.at[b], tables.at[b], t_send.at[b], t_recv.at[b], "expert", me
                ).wait_recv()

                @pl.when(passes(side))
                def _():
                    hop(None, side, d).start()

        loop(low, high, take)
        loop(low, high, lambda side: forward(source(side)))

        def back(side):
            b = source(side)
            hid[...] = jnp.zeros_like(hid)

            def part(q):
                @pl.when(d > 0)
                def _():
                    arrival(q, side, d - 1).wait_recv()

                    @pl.when(passes(side))
                    def _():
                        hop(q, side, d).start()

                gather_hidden(b, q)

            loop(0, PIECES, part)
            slopes(b)
            loop(0, feature // WIDE, functools.partial(input_tile, b))

            @pl.when(jnp.logical_and(is_end, d > 0))
            def _():
                send_rows(b)

        @pl.when(d < n - 1)
        def _():
            loop(low, high, back)

    loop(0, n, distance)

    if fold:

        @pl.when(is_mid)
        def _():
            fold_copy().start()
            send_rows(ally)

    else:
        for target in others:
            inner = jnp.logical_and(target > 0, target < n - 1)

            @pl.when(jnp.logical_and(is_mid, inner))
            def _():
                send_rows(target)

    def place_of(way, who):
        value = 0
        for i, b in enumerate(orders[way]):
            value = value + lax.rem(who // (1 << b), 2) * (1 << (bits - 1 - i))
        return value

    kinds = {
        "both": (both_part, both_got, b_send, b_recv),
        "down": (down_part, down_got, d_send, d_recv),
    }

    def base(way, i):
        value = 0
        for j in range(i):
            value = value + bit[orders[way][j]] * (replicas >> (j + 1))
        return value

    def stage(kind, c, way, i):
        part, got, send, recv = kinds[kind]
        b = orders[way][i]
        count = replicas >> (i + 1)
        start = base(way, i) + (1 - bit[b]) * count
        pick = slice(None) if i == 0 else way
        return remote(
            part.at[c, pick, pl.ds(start, count)],
            got[i].at[c, pick],
            send.at[c, i, way],
            recv.at[c, i, way],
            "dp",
            mate[b],
        )

    def combine(kind, c, i):
        part, got, _, _ = kinds[kind]
        count = replicas >> (i + 1)
        if i == 0:
            stage(kind, c, 0, 0).wait_recv()
        for way in range(2):
            start = base(way, i + 1)
            if i > 0:
                stage(kind, c, way, i).wait_recv()
            if i == bits - 1:
                total = part[c, way, start].astype(F32) + got[i][c, way, 0].astype(F32)
                if kind == "both":
                    both_out[:, span(2 * c + way, TILE // 2)] = total.astype(BF16)
                else:
                    down_out[:, span(2 * c + way, piece // 2)] = total.astype(BF16)
                continue

            def add(k):
                total = part[c, way, start + k].astype(F32) + got[i][c, way, k].astype(F32)
                part[c, way, start + k] = total.astype(BF16)

            loop(0, count, add)
            stage(kind, c, way, i + 1).start()

    def spread(kind, c, who, value):
        part = kinds[kind][0]
        size = value.shape[1] // 2
        for way in range(2):
            half_value = value[:, way * size : (way + 1) * size]
            part[c, way, place_of(way, who)] = half_value.astype(BF16)

    def both_chunk(c):
        def place(side, j):
            who = 2 * j + side
            lines = span(who, both_rows)
            value = jnp.dot(x_t[lines, :], pair_d[:, span(c, TILE)], preferred_element_type=F32)
            spread("both", c, who, value)

        loop(0, half, functools.partial(place, 1 - bit[0]), unroll=2)
        stage("both", c, 0, 0).start()
        loop(0, half, functools.partial(place, bit[0]), unroll=2)

    def down_chunk(q):
        cols = span(q, piece)
        group = 1 if down_rows % 16 == 0 else 2

        def place(side, j):
            who = 2 * j + side
            lines = span(who // group, group * down_rows)
            value = jnp.dot(h_t[lines, :], dy_all[:, cols], preferred_element_type=F32)
            for k in range(group):
                spread("down", q, who + k, value[k * down_rows : (k + 1) * down_rows])

        if group == 1:
            loop(0, half, functools.partial(place, 1 - bit[0]), unroll=2)
            stage("down", q, 0, 0).start()
            loop(0, half, functools.partial(place, bit[0]), unroll=2)
        else:
            loop(0, half, functools.partial(place, 0))
            stage("down", q, 0, 0).start()

    last = jnp.clip(n - 1 - me, 0, n - 1)
    last_side = jnp.where(me == n - 1, 0, 1)

    @pl.when(is_end)
    def _():
        hid[...] = jnp.zeros_like(hid)

    def early(q):
        @pl.when(q > 0)
        def _():
            combine("down", q - 1, 0)

        @pl.when(is_end)
        def _():
            arrival(q, last_side, n - 2).wait_recv()
            gather_hidden(last, q)

            @pl.when(q == PIECES - 1)
            def _():
                slopes(last)

        down_chunk(q)

        @pl.when(q > 1)
        def _():
            combine("down", q - 2, 1)

    loop(0, PIECES, early)
    wide = feature // WIDE

    def late(c):
        both_chunk(c)

        @pl.when(c == 0)
        def _():
            combine("down", PIECES - 1, 0)

        @pl.when(c > 0)
        def _():
            combine("both", c - 1, 0)

        for t in range(2):
            j = 2 * (c - 1) + t

            @pl.when(jnp.logical_and(is_end, jnp.logical_and(c > 0, j < wide)))
            def _():
                input_tile(last, j)

                @pl.when(j == wide - 1)
                def _():
                    send_rows(last)

        for k in range(2):

            @pl.when(c == 1 + 2 * k)
            def _():
                combine("down", PIECES - 2 + k, 1)

    loop(0, chunks, late)
    combine("both", chunks - 1, 0)

    for side in range(2):
        for s in range(n - 1):

            @pl.when(sends(side, s))
            def _():
                hop(None, side, s).wait_send()
                for p in range(PIECES):
                    hop(p, side, s).wait_send()

    if fold:

        @pl.when(is_mid)
        def _():
            folded().wait_recv()

            def add(j):
                cols = span(j, TILE)
                total = rows_out[near, :, cols].astype(F32) + rows_got[me, :, cols].astype(F32)
                rows_out[near, :, cols] = total.astype(BF16)

            loop(0, feature // TILE, add)
            row_copy(near).start()
            comb_copy(near).start()
            comb_copy(far).start()

    else:
        for target in others:
            outer = jnp.logical_or(target == 0, target == n - 1)

            @pl.when(jnp.logical_and(is_mid, outer))
            def _():
                send_rows(target)

    for i in range(1, bits - 1):
        if i > 1:
            loop(0, PIECES, lambda q: combine("down", q, i))
        loop(0, chunks, lambda c: combine("both", c, i))

    loop(0, PIECES, lambda q: combine("down", q, bits - 1))

    def takes_row(b):
        if not fold:
            return b >= 0
        return jnp.logical_or(is_mid, b != jnp.where(me == 0, n - 2, 1))

    def gives_row(target):
        if not fold:
            return target >= 0
        return jnp.logical_or(is_end, target != far)

    for b in others:

        @pl.when(takes_row(b))
        def _():
            remote(
                rows_got.at[b], rows_got.at[b], r_send.at[b], r_recv.at[b], "expert", me
            ).wait_recv()

        remote(
            comb_got.at[b], comb_got.at[b], c_send.at[b], c_recv.at[b], "expert", me
        ).wait_recv()

    def total_rows(who):
        def tile(j):
            cols = span(j, TILE)
            total = rows_out[me, :, cols].astype(F32)
            for b in who:
                total = total + rows_got[b, :, cols].astype(F32)
            in_grad[:, cols] = total.astype(BF16)

        loop(0, feature // TILE, tile)

    if fold:

        @pl.when(is_end)
        def _():
            total_rows([n - 1 - me, jnp.where(me == 0, 1, n - 2)])

        @pl.when(is_mid)
        def _():
            total_rows(others)

    else:
        total_rows(others)

    picked = jnp.where(ids[...] == me, comb_out[me, 0:1, :], 0.0)
    for b in others:
        picked = picked + jnp.where(ids[...] == b, comb_got[b, 0:1, :], 0.0)
    comb_grad[...] = picked

    loop(0, chunks, lambda c: combine("both", c, bits - 1))

    for target in others:
        table_copy(target).wait_send()
        comb_copy(target).wait_send()

        @pl.when(gives_row(target))
        def _():
            row_copy(target).wait_send()

    if fold:

        @pl.when(is_mid)
        def _():
            fold_copy().wait_send()

    for kind, count in (("both", chunks), ("down", PIECES)):

        def drain(c):
            stage(kind, c, 0, 0).wait_send()
            for way in range(2):
                for i in range(1, bits):
                    stage(kind, c, way, i).wait_send()

        loop(0, count, drain)


def deliver_kernel(rows, comb, both, down, *refs):
    outs, sems = refs[:-1], refs[-1]
    width = outs[2].shape[2]
    copies = []
    for src, dst in (
        (rows, outs[0]),
        (both.at[:, pl.ds(0, width)], outs[2].at[0]),
        (both.at[:, pl.ds(width, width)], outs[3].at[0]),
        (down, outs[4].at[0]),
        (comb, outs[1]),
    ):
        copies.append(pltpu.make_async_copy(src, dst, sems.at[len(copies)]))
        copies[-1].start()
    for copy in copies:
        copy.wait()


def deliver(rows, comb, both, down):
    width = both.shape[1] // 2
    outs = [
        jax.ShapeDtypeStruct(rows.shape, BF16),
        jax.ShapeDtypeStruct(comb.shape, F32),
        jax.ShapeDtypeStruct((1, both.shape[0], width), BF16),
        jax.ShapeDtypeStruct((1, both.shape[0], width), BF16),
        jax.ShapeDtypeStruct((1,) + down.shape, BF16),
    ]
    input_grad, combine_grad, gate_grad, up_grad, down_grad = pl.pallas_call(
        deliver_kernel,
        out_shape=outs,
        in_specs=[VMEM] * 4,
        out_specs=[HBM] * 5,
        scratch_shapes=[pltpu.SemaphoreType.DMA((5,))],
        compiler_params=pltpu.CompilerParams(vmem_limit_bytes=8 * 1024 * 1024),
        name="deliver",
    )(rows, comb, both, down)
    return (input_grad, combine_grad.T, gate_grad, up_grad, down_grad)


def shards(tokens, cotangent, expert_ids, combine, w_gate, w_up, w_down):
    n = lax.axis_size("expert")
    replicas = lax.axis_size("dp")
    bits = replicas.bit_length() - 1
    rows, top = expert_ids.shape
    feature = tokens.shape[1]
    width = w_gate.shape[2]
    everyone = n * rows
    chunks = 2 * width // TILE
    piece = feature // PIECES
    both_rows, down_rows = feature // replicas, width // replicas
    table = -(-n // 8) * 8
    outs = [
        jax.ShapeDtypeStruct((rows, feature), BF16),
        jax.ShapeDtypeStruct((top, rows), F32),
        jax.ShapeDtypeStruct((both_rows, 2 * width), BF16),
        jax.ShapeDtypeStruct((down_rows, feature), BF16),
    ]
    scratch = [
        pltpu.VMEM((everyone, feature), BF16),
        pltpu.VMEM((everyone, feature), BF16),
        pltpu.VMEM((feature, everyone), BF16),
        pltpu.VMEM((feature, width), BF16),
        pltpu.VMEM((feature, width), BF16),
        pltpu.VMEM((width, feature), BF16),
        pltpu.VMEM((everyone, width), F32),
        pltpu.VMEM((everyone, width), F32),
        pltpu.VMEM((everyone, width), BF16),
        pltpu.VMEM((width, everyone), BF16),
        pltpu.VMEM((everyone, 2 * width), BF16),
        pltpu.VMEM((rows, width), F32),
        pltpu.VMEM((n, rows, feature), BF16),
        pltpu.VMEM((n, rows, feature), BF16),
        pltpu.VMEM((n, table, rows), F32),
        pltpu.VMEM((n, 8, rows), F32),
        pltpu.VMEM((n, 8, rows), F32),
        pltpu.VMEM((chunks, 2, replicas, both_rows, TILE // 2), BF16),
        pltpu.VMEM((PIECES, 2, replicas, down_rows, piece // 2), BF16),
    ]
    for i in range(bits):
        count = replicas >> (i + 1)
        scratch.append(pltpu.VMEM((chunks, 2, count, both_rows, TILE // 2), BF16))
    for i in range(bits):
        count = replicas >> (i + 1)
        scratch.append(pltpu.VMEM((PIECES, 2, count, down_rows, piece // 2), BF16))
    scratch += [pltpu.SemaphoreType.DMA((3,))]
    scratch += [pltpu.SemaphoreType.DMA((1 + PIECES, 2, n))] * 2
    scratch += [pltpu.SemaphoreType.DMA((n,))] * 6
    scratch += [pltpu.SemaphoreType.DMA((chunks, bits, 2))] * 2
    scratch += [pltpu.SemaphoreType.DMA((PIECES, bits, 2))] * 2
    scratch += [pltpu.SemaphoreType.DMA((1,))] * 2
    input_grad, combine_grad, both, down = pl.pallas_call(
        functools.partial(layer_kernel, n, bits),
        out_shape=outs,
        in_specs=[VMEM] * 4 + [HBM] * 3,
        out_specs=[VMEM] * 4,
        scratch_shapes=scratch,
        compiler_params=pltpu.CompilerParams(
            collective_id=0, has_side_effects=True, vmem_limit_bytes=LIMIT
        ),
        name="layer",
    )(expert_ids.T, combine.T, tokens, cotangent, w_gate, w_up, w_down)
    return deliver(input_grad, combine_grad, both, down)


def solution(mesh):
    by_token = P(("dp", "expert"), None)
    by_expert = P("expert", None, None)
    by_row = P("expert", "dp", None)
    return jax.shard_map(
        shards,
        mesh=mesh,
        in_specs=(by_token,) * 4 + (by_expert,) * 3,
        out_specs=(by_token, by_token, by_row, by_row, by_row),
        check_vma=False,
    )
```

```python
import functools
import jax
import jax.numpy as jnp
from jax import lax
from jax.experimental import pallas as pl
from jax.experimental.pallas import tpu as pltpu
from jax.sharding import PartitionSpec as P

MESH = pl.DeviceIdType.MESH
VMEM = pl.BlockSpec(memory_space=pltpu.VMEM)
HBM = pl.BlockSpec(memory_space=pltpu.HBM)
LIMIT = 50 * 1024 * 1024
TILE = 256
WIDE = 512
PIECES = 4
LAST = (((1,), (1,)), ((), ()))
F32 = jnp.float32
BF16 = jnp.bfloat16


def remote(src, dst, send, recv, axis, target):
    return pltpu.make_async_remote_copy(
        src_ref=src,
        dst_ref=dst,
        send_sem=send,
        recv_sem=recv,
        device_id={axis: target},
        device_id_type=MESH,
    )


def span(index, size):
    return pl.ds(pl.multiple_of(index * size, size), size)


def loop(low, high, body, **options):
    def step(i, carry):
        body(i)
        return carry

    lax.fori_loop(low, high, step, 0, **options)


def layer_kernel(n, bits, *refs):
    ids, comb, x_in, dy_in, g_in, u_in, d_in = refs[:7]
    in_grad, comb_grad, both_out, down_out = refs[7:11]
    x_all, dy_all, x_t, wg, wu, wd, slope, act_all = refs[11:19]
    h_all, h_t, pair_d, hid, rows_out, rows_got = refs[19:25]
    tables, comb_out, comb_got, h_guest, down_guest = refs[25:30]
    both_part, down_part = refs[30:32]
    both_got, down_got = refs[32 : 32 + bits], refs[32 + bits : 32 + 2 * bits]
    rest = refs[32 + 2 * bits :]
    load, a_send, a_recv, t_send, t_recv, r_send, r_recv, c_send, c_recv = rest[:9]
    b_send, b_recv, d_send, d_recv, f_send, f_recv, h_send, h_recv = rest[9:17]

    me = lax.axis_index("expert")
    rank = lax.axis_index("dp")
    replicas = 1 << bits
    half = replicas // 2
    rows = in_grad.shape[0]
    feature, width = wg.shape
    piece = feature // PIECES
    chunks = 2 * width // TILE
    both_rows, down_rows = both_out.shape[0], down_out.shape[0]
    bit = [lax.rem(rank // (1 << b), 2) for b in range(bits)]
    mate = [rank + (1 - 2 * bit[b]) * (1 << b) for b in range(bits)]
    orders = ([0] + list(range(1, bits)), [0] + list(range(bits - 1, 0, -1)))
    is_end = jnp.logical_or(me == 0, me == n - 1)
    is_mid = jnp.logical_not(is_end)

    loads = [
        pltpu.make_async_copy(src, dst, load.at[i])
        for i, (src, dst) in enumerate(
            (
                (g_in.at[0], wg),
                (u_in.at[0], wu),
                (d_in.at[0], wd),
            )
        )
    ]
    for item in loads:
        item.start()
    barrier = pltpu.get_barrier_semaphore()
    for k in range(1, n):
        pl.semaphore_signal(
            barrier, inc=1, device_id={"expert": lax.rem(me + k, n)}, device_id_type=MESH
        )
    for b in range(bits):
        pl.semaphore_signal(barrier, inc=1, device_id={"dp": mate[b]}, device_id_type=MESH)

    expert = lax.broadcasted_iota(jnp.int32, tables.shape[1:], 0)
    weight = jnp.where(expert == ids[0:1, :], comb[0:1, :], 0.0)
    for k in range(1, ids.shape[0]):
        weight = weight + jnp.where(expert == ids[k : k + 1, :], comb[k : k + 1, :], 0.0)
    tables[me] = weight

    def view(p, block):
        if p is None:
            return x_all.at[span(block, rows)]
        return dy_all.at[span(block, rows), span(p, piece)]

    def index(p):
        return 0 if p is None else 1 + p

    def hop(p, side, s, own=False):
        step = 1 - 2 * side
        slot = view(p, jnp.clip(me - step * s, 0, n - 1))
        target = jnp.clip(me + step, 0, n - 1)
        i = index(p)
        src = slot
        if own:
            src = x_in if p is None else dy_in.at[:, span(p, piece)]
        return remote(src, slot, a_send.at[i, side, s], a_recv.at[i, side, s], "expert", target)

    def arrival(p, side, s):
        step = 1 - 2 * side
        slot = view(p, jnp.clip(me - step * (s + 1), 0, n - 1))
        i = index(p)
        return remote(slot, slot, a_send.at[i, side, s], a_recv.at[i, side, s], "expert", me)

    def sends(side, s):
        if side == 0:
            return jnp.logical_and(me >= s, me + 1 < n)
        return jnp.logical_and(me + s < n, me >= 1)

    def passes(side):
        return jnp.where(side == 0, me + 1 < n, me >= 1)

    def table_copy(target):
        return remote(
            tables.at[me], tables.at[me], t_send.at[target], t_recv.at[me], "expert", target
        )

    def row_copy(target):
        return remote(
            rows_out.at[target],
            rows_got.at[me],
            r_send.at[target],
            r_recv.at[me],
            "expert",
            target,
        )

    def tile_copy(target, j):
        cols = span(j, WIDE)
        return remote(
            rows_out.at[target, :, cols],
            rows_got.at[me, :, cols],
            r_send.at[target],
            r_recv.at[me],
            "expert",
            target,
        )

    fold = n == 4
    ally = n - 1 - me
    near = jnp.where(2 * me < n, 0, n - 1)
    far = n - 1 - near

    shared = PIECES - 1 if fold else PIECES
    helper = jnp.where(me == 0, 1, n - 2)
    own_down = PIECES
    if fold:
        own_down = jnp.where(is_end, shared, PIECES + 1)

    def hidden_copy(b):
        cols = span(b, rows)
        return remote(
            h_t.at[:, cols], h_guest.at[:, cols], h_send.at[b], h_recv.at[b], "expert", helper
        )

    def guest_copy():
        return remote(
            down_guest,
            down_out.at[:, span(PIECES - 1, piece)],
            f_send.at[1],
            f_recv.at[1],
            "expert",
            near,
        )

    def fold_copy():
        return remote(
            rows_out.at[far], rows_got.at[ally], f_send.at[0], f_recv.at[0], "expert", ally
        )

    def folded():
        slot = rows_got.at[me]
        return remote(slot, slot, f_send.at[0], f_recv.at[0], "expert", me)

    def comb_copy(target):
        return remote(
            comb_out.at[target],
            comb_got.at[me],
            c_send.at[target],
            c_recv.at[me],
            "expert",
            target,
        )

    pl.semaphore_wait(barrier, n - 1 + bits)
    others = [lax.rem(me + k, n) for k in range(1, n)]
    for target in others:
        table_copy(target).start()
    for p in [None] + list(range(PIECES)):
        for side in range(2):
            ready = sends(side, 0)
            if p is not None and p > 0:
                ready = jnp.logical_and(ready, me == (0, n - 1)[side])

            @pl.when(ready)
            def _():
                hop(p, side, 0, True).start()

    x_all[span(me, rows), :] = x_in[...]
    dy_all[span(me, rows), :] = dy_in[...]
    for item in loads:
        item.wait()

    def coefficient(b):
        line = tables[b, pl.ds(me, 1), :]
        return jnp.broadcast_to(line, (128, rows)).T[:, 0:1]

    def forward(b):
        own = span(b, rows)
        coef = coefficient(b)

        def tile(j):
            cols = span(j, TILE)
            value = x_all[own, :]
            gate = jnp.dot(value, wg[:, cols], preferred_element_type=F32)
            up = jnp.dot(value, wu[:, cols], preferred_element_type=F32)
            sig = jax.nn.sigmoid(gate)
            act = gate * sig
            hidden = (act * up).astype(BF16)
            slope[own, cols] = up * (sig * (1.0 + gate * (1.0 - sig)))
            act_all[own, cols] = act
            h_all[own, cols] = hidden
            h_t[cols, own] = (coef * hidden.astype(F32)).T.astype(BF16)

        loop(0, width // TILE, tile)

        def turn(j):
            cols = span(j, TILE)
            x_t[cols, own] = x_all[own, cols].T

        if fold:

            @pl.when(is_end)
            def _():
                hidden_copy(b).start()

        loop(0, feature // TILE, turn)

    def gather_hidden(b, q, slot=0):
        cols = span(q, piece)
        hid[slot] += lax.dot_general(
            dy_all[span(b, rows), cols], wd[:, cols], LAST, preferred_element_type=F32
        )

    def slopes(b, slot=0):
        own = span(b, rows)
        coef = coefficient(b)

        def tile(j, total):
            cols = span(j, TILE)
            grad = hid[slot, :, cols]
            total = total + jnp.sum(h_all[own, cols].astype(F32) * grad, axis=1, keepdims=True)
            grad = coef * grad
            pair_d[own, cols] = (grad * slope[own, cols]).astype(BF16)
            pair_d[own, span(width // TILE + j, TILE)] = (grad * act_all[own, cols]).astype(BF16)
            return total

        total = lax.fori_loop(0, width // TILE, tile, jnp.zeros((rows, 1), F32))
        comb_out[b] = jnp.broadcast_to(total, (rows, 128)).T[:8]

    def input_tile(b, j):
        own = span(b, rows)
        cols = span(j, WIDE)
        value = lax.dot_general(pair_d[own, :width], wg[cols, :], LAST, preferred_element_type=F32)
        value = value + lax.dot_general(
            pair_d[own, width:], wu[cols, :], LAST, preferred_element_type=F32
        )
        rows_out[b, :, cols] = value.astype(BF16)

    def send_rows(b):
        row_copy(b).start()
        comb_copy(b).start()

    def first(d):
        return jnp.where(jnp.logical_or(d == 0, me >= d), 0, 1)

    def bound(d):
        return jnp.where(jnp.logical_and(d > 0, me + d < n), 2, 1)

    def source(side, d):
        return jnp.clip(me + d * (2 * side - 1), 0, n - 1)

    def by_end(side):
        return jnp.where(side == 0, me == n - 2, me == 1)

    def back(b, d):
        hid[0] = jnp.zeros(hid.shape[1:], F32)
        loop(0, PIECES, lambda q: gather_hidden(b, q))
        slopes(b)
        loop(0, feature // WIDE, functools.partial(input_tile, b))

        @pl.when(jnp.logical_and(is_end, d > 0))
        def _():
            send_rows(b)

    def distance(d):
        def take(side):
            @pl.when(d > 0)
            def _():
                arrival(None, side, d - 1).wait_recv()
                b = source(side, d)
                remote(
                    tables.at[b], tables.at[b], t_send.at[b], t_recv.at[b], "expert", me
                ).wait_recv()

                @pl.when(passes(side))
                def _():
                    hop(None, side, d).start()

                    @pl.when(d == 1)
                    def _():
                        for p in range(1, PIECES):
                            hop(p, side, 0, True).start()

        loop(first(d), bound(d), take)
        loop(first(d), bound(d), lambda side: forward(source(side, d)))
        e = jnp.maximum(d - 1, 0)

        def take_piece(i):
            q, side = i // 2, lax.rem(i, 2)
            here = jnp.logical_and(side >= first(e), side < bound(e))

            @pl.when(jnp.logical_and(here, e > 0))
            def _():
                arrival(q, side, e - 1).wait_recv()
                later = jnp.logical_and(by_end(side), e == n - 3)

                @pl.when(jnp.logical_and(passes(side), jnp.logical_not(later)))
                def _():
                    hop(q, side, e).start()

        @pl.when(jnp.logical_or(d == 0, jnp.logical_and(d > 1, d < n - 1)))
        def _():
            loop(0, 2 * PIECES, take_piece)
            loop(first(e), bound(e), lambda side: back(source(side, e), e))

    loop(0, n, distance)

    @pl.when(jnp.logical_or(me == 1, me == n - 2))
    def _():
        side = jnp.where(me == 1, 1, 0)

        def take(q):
            arrival(q, side, n - 3).wait_recv()
            hop(q, side, n - 3).start()
            hop(q, side, n - 2).start()

        loop(0, PIECES, take)
        back(source(side, n - 2), n - 2)

    if fold:

        @pl.when(is_mid)
        def _():
            fold_copy().start()
            send_rows(ally)

    else:
        for target in others:
            inner = jnp.logical_and(target > 0, target < n - 1)

            @pl.when(jnp.logical_and(is_mid, inner))
            def _():
                send_rows(target)

    def place_of(way, who):
        value = 0
        for i, b in enumerate(orders[way]):
            value = value + lax.rem(who // (1 << b), 2) * (1 << (bits - 1 - i))
        return value

    kinds = {
        "both": (both_part, both_got, b_send, b_recv),
        "down": (down_part, down_got, d_send, d_recv),
    }

    def base(way, i):
        value = 0
        for j in range(i):
            value = value + bit[orders[way][j]] * (replicas >> (j + 1))
        return value

    def stage(kind, c, way, i):
        part, got, send, recv = kinds[kind]
        b = orders[way][i]
        count = replicas >> (i + 1)
        start = base(way, i) + (1 - bit[b]) * count
        pick = slice(None) if i == 0 else way
        return remote(
            part.at[c, pick, pl.ds(start, count)],
            got[i].at[c, pick],
            send.at[c, i, way],
            recv.at[c, i, way],
            "dp",
            mate[b],
        )

    def combine(kind, c, i):
        part, got, _, _ = kinds[kind]
        count = replicas >> (i + 1)
        if i == 0:
            stage(kind, c, 0, 0).wait_recv()
        for way in range(2):
            start = base(way, i + 1)
            if i > 0:
                stage(kind, c, way, i).wait_recv()
            if i == bits - 1:
                total = part[c, way, start].astype(F32) + got[i][c, way, 0].astype(F32)
                if kind == "both":
                    both_out[:, span(2 * c + way, TILE // 2)] = total.astype(BF16)
                elif fold:

                    @pl.when(c < PIECES)
                    def _():
                        down_out[:, span(2 * c + way, piece // 2)] = total.astype(BF16)

                    @pl.when(c == PIECES)
                    def _():
                        down_guest[:, span(way, piece // 2)] = total.astype(BF16)

                else:
                    down_out[:, span(2 * c + way, piece // 2)] = total.astype(BF16)
                continue

            def add(k):
                total = part[c, way, start + k].astype(F32) + got[i][c, way, k].astype(F32)
                part[c, way, start + k] = total.astype(BF16)

            loop(0, count, add)
            stage(kind, c, way, i + 1).start()

    def spread(kind, c, who, value):
        part = kinds[kind][0]
        size = value.shape[1] // 2
        for way in range(2):
            half_value = value[:, way * size : (way + 1) * size]
            part[c, way, place_of(way, who)] = half_value.astype(BF16)

    def both_chunk(c):
        def place(side, j):
            who = 2 * j + side
            lines = span(who, both_rows)
            value = jnp.dot(x_t[lines, :], pair_d[:, span(c, TILE)], preferred_element_type=F32)
            spread("both", c, who, value)

        loop(0, half, functools.partial(place, 1 - bit[0]), unroll=2)
        stage("both", c, 0, 0).start()
        loop(0, half, functools.partial(place, bit[0]), unroll=2)

    def down_chunk(q, held=h_t):
        cols = span(min(q, PIECES - 1) if isinstance(q, int) else q, piece)
        group = 1 if down_rows % 16 == 0 else 2

        def place(side, j):
            who = 2 * j + side
            lines = span(who // group, group * down_rows)
            value = jnp.dot(held[lines, :], dy_all[:, cols], preferred_element_type=F32)
            for k in range(group):
                spread("down", q, who + k, value[k * down_rows : (k + 1) * down_rows])

        if group == 1:
            loop(0, half, functools.partial(place, 1 - bit[0]), unroll=2)
            stage("down", q, 0, 0).start()
            loop(0, half, functools.partial(place, bit[0]), unroll=2)
        else:
            loop(0, half, functools.partial(place, 0))
            stage("down", q, 0, 0).start()

    last = jnp.clip(n - 1 - me, 0, n - 1)
    prior = jnp.where(me == n - 1, 1, n - 2)
    last_side = jnp.where(me == n - 1, 0, 1)

    @pl.when(is_end)
    def _():
        hid[...] = jnp.zeros_like(hid)

    wide = feature // WIDE

    def last_tile(j):
        @pl.when(jnp.logical_and(is_end, j < 2 * wide))
        def _():
            b = jnp.where(j < wide, last, prior)
            tile = lax.rem(j, wide)
            input_tile(b, tile)
            tile_copy(b, tile).start()

            @pl.when(tile == wide - 1)
            def _():
                comb_copy(b).start()

    def early(q):
        @pl.when(is_end)
        def _():
            for slot, b in enumerate((prior, last)):
                arrival(q, last_side, n - 3 + slot).wait_recv()
                gather_hidden(b, q, slot)

        down_chunk(q)
        combine("down", q, 0)

        @pl.when(q > 0)
        def _():
            combine("down", q - 1, 1)

    loop(0, PIECES - 1, early)

    @pl.when(is_end)
    def _():
        for slot, b in enumerate((prior, last)):
            arrival(PIECES - 1, last_side, n - 3 + slot).wait_recv()
            gather_hidden(b, PIECES - 1, slot)
            slopes(b, slot)

    if fold:

        @pl.when(is_mid)
        def _():
            for b in range(n):
                cols = span(b, rows)
                slot = h_guest.at[:, cols]
                remote(slot, slot, h_send.at[b], h_recv.at[b], "expert", me).wait_recv()
            down_chunk(PIECES, h_guest)

    both_chunk(0)
    both_chunk(1)
    combine("both", 0, 0)
    combine("down", PIECES - 2, 1)
    last_tile(0)
    combine("both", 1, 0)

    def rest_down(i):
        if i == 0:
            down_chunk(PIECES - 1)
            if fold:
                combine("down", PIECES, 0)
        combine("down", PIECES - 1, i)
        if fold and i > 0:
            combine("down", PIECES, i)

    def when_owned(body):
        if fold:
            pl.when(is_mid)(body)
        else:
            body()

    when_owned(lambda: rest_down(0))
    last_tile(1)
    last_tile(2)

    def settle():
        for side in range(2):
            for s in range(n - 1):

                @pl.when(sends(side, s))
                def _():
                    hop(None, side, s).wait_send()
                    for p in range(PIECES):
                        hop(p, side, s).wait_send()

        if fold:

            @pl.when(is_mid)
            def _():
                folded().wait_recv()

                def add(j):
                    cols = span(j, TILE)
                    total = rows_out[near, :, cols].astype(F32) + rows_got[me, :, cols].astype(F32)
                    rows_out[near, :, cols] = total.astype(BF16)

                loop(0, feature // TILE, add)
                row_copy(near).start()
                comb_copy(near).start()
                comb_copy(far).start()

        else:
            for target in others:
                outer = jnp.logical_or(target == 0, target == n - 1)

                @pl.when(jnp.logical_and(is_mid, outer))
                def _():
                    send_rows(target)

    def late(c):
        both_chunk(c)
        for t in range(2):
            last_tile(2 * c - 1 + t)
        combine("both", c, 0)

        @pl.when(c == 3)
        def _():
            when_owned(lambda: rest_down(1))

        @pl.when(c == 2)
        def _():
            settle()

    loop(2, chunks, late)

    for i in range(1, bits - 1):
        if i > 1:
            loop(0, own_down, lambda q: combine("down", q, i))
        loop(0, chunks, lambda c: combine("both", c, i))

    loop(0, own_down, lambda q: combine("down", q, bits - 1))
    if fold:

        @pl.when(is_mid)
        def _():
            guest_copy().start()


    def takes_row(b):
        if not fold:
            return b >= 0
        return jnp.logical_or(is_mid, b != jnp.where(me == 0, n - 2, 1))

    def gives_row(target):
        if not fold:
            return target >= 0
        return jnp.logical_or(is_end, target != far)

    for b in others:

        @pl.when(takes_row(b))
        def _():
            remote(
                rows_got.at[b], rows_got.at[b], r_send.at[b], r_recv.at[b], "expert", me
            ).wait_recv()

        remote(
            comb_got.at[b], comb_got.at[b], c_send.at[b], c_recv.at[b], "expert", me
        ).wait_recv()

    def total_rows(who):
        def tile(j):
            cols = span(j, TILE)
            total = rows_out[me, :, cols].astype(F32)
            for b in who:
                total = total + rows_got[b, :, cols].astype(F32)
            in_grad[:, cols] = total.astype(BF16)

        loop(0, feature // TILE, tile)

    if fold:

        @pl.when(is_end)
        def _():
            total_rows([n - 1 - me, jnp.where(me == 0, 1, n - 2)])

        @pl.when(is_mid)
        def _():
            total_rows(others)

    else:
        total_rows(others)

    picked = jnp.where(ids[...] == me, comb_out[me, 0:1, :], 0.0)
    for b in others:
        picked = picked + jnp.where(ids[...] == b, comb_got[b, 0:1, :], 0.0)
    comb_grad[...] = picked

    loop(0, chunks, lambda c: combine("both", c, bits - 1))

    if fold:

        @pl.when(is_end)
        def _():
            slot = down_out.at[:, span(PIECES - 1, piece)]
            remote(slot, slot, f_send.at[1], f_recv.at[1], "expert", me).wait_recv()
            for b in range(n):
                hidden_copy(b).wait_send()

        @pl.when(is_mid)
        def _():
            guest_copy().wait_send()

    for target in others:
        table_copy(target).wait_send()
        comb_copy(target).wait_send()

        @pl.when(gives_row(target))
        def _():
            row_copy(target).wait_send()

    if fold:

        @pl.when(is_mid)
        def _():
            fold_copy().wait_send()

    for kind, count in (("both", chunks), ("down", own_down)):

        def drain(c):
            stage(kind, c, 0, 0).wait_send()
            for way in range(2):
                for i in range(1, bits):
                    stage(kind, c, way, i).wait_send()

        loop(0, count, drain)


def deliver_kernel(rows, comb, both, down, *refs):
    outs, sems = refs[:-1], refs[-1]
    width = outs[2].shape[2]
    copies = []
    for src, dst in (
        (rows, outs[0]),
        (both.at[:, pl.ds(0, width)], outs[2].at[0]),
        (both.at[:, pl.ds(width, width)], outs[3].at[0]),
        (down, outs[4].at[0]),
        (comb, outs[1]),
    ):
        copies.append(pltpu.make_async_copy(src, dst, sems.at[len(copies)]))
        copies[-1].start()
    for copy in copies:
        copy.wait()


def deliver(rows, comb, both, down):
    width = both.shape[1] // 2
    outs = [
        jax.ShapeDtypeStruct(rows.shape, BF16),
        jax.ShapeDtypeStruct(comb.shape, F32),
        jax.ShapeDtypeStruct((1, both.shape[0], width), BF16),
        jax.ShapeDtypeStruct((1, both.shape[0], width), BF16),
        jax.ShapeDtypeStruct((1,) + down.shape, BF16),
    ]
    input_grad, combine_grad, gate_grad, up_grad, down_grad = pl.pallas_call(
        deliver_kernel,
        out_shape=outs,
        in_specs=[VMEM] * 4,
        out_specs=[HBM] * 5,
        scratch_shapes=[pltpu.SemaphoreType.DMA((5,))],
        compiler_params=pltpu.CompilerParams(vmem_limit_bytes=8 * 1024 * 1024),
        name="deliver",
    )(rows, comb, both, down)
    return (input_grad, combine_grad.T, gate_grad, up_grad, down_grad)


def shards(tokens, cotangent, expert_ids, combine, w_gate, w_up, w_down):
    n = lax.axis_size("expert")
    replicas = lax.axis_size("dp")
    bits = replicas.bit_length() - 1
    rows, top = expert_ids.shape
    feature = tokens.shape[1]
    width = w_gate.shape[2]
    everyone = n * rows
    chunks = 2 * width // TILE
    piece = feature // PIECES
    both_rows, down_rows = feature // replicas, width // replicas
    table = -(-n // 8) * 8
    outs = [
        jax.ShapeDtypeStruct((rows, feature), BF16),
        jax.ShapeDtypeStruct((top, rows), F32),
        jax.ShapeDtypeStruct((both_rows, 2 * width), BF16),
        jax.ShapeDtypeStruct((down_rows, feature), BF16),
    ]
    scratch = [
        pltpu.VMEM((everyone, feature), BF16),
        pltpu.VMEM((everyone, feature), BF16),
        pltpu.VMEM((feature, everyone), BF16),
        pltpu.VMEM((feature, width), BF16),
        pltpu.VMEM((feature, width), BF16),
        pltpu.VMEM((width, feature), BF16),
        pltpu.VMEM((everyone, width), F32),
        pltpu.VMEM((everyone, width), F32),
        pltpu.VMEM((everyone, width), BF16),
        pltpu.VMEM((width, everyone), BF16),
        pltpu.VMEM((everyone, 2 * width), BF16),
        pltpu.VMEM((2, rows, width), F32),
        pltpu.VMEM((n, rows, feature), BF16),
        pltpu.VMEM((n, rows, feature), BF16),
        pltpu.VMEM((n, table, rows), F32),
        pltpu.VMEM((n, 8, rows), F32),
        pltpu.VMEM((n, 8, rows), F32),
        pltpu.VMEM((width, everyone), BF16),
        pltpu.VMEM((down_rows, piece), BF16),
        pltpu.VMEM((chunks, 2, replicas, both_rows, TILE // 2), BF16),
        pltpu.VMEM((PIECES + 1, 2, replicas, down_rows, piece // 2), BF16),
    ]
    for i in range(bits):
        count = replicas >> (i + 1)
        scratch.append(pltpu.VMEM((chunks, 2, count, both_rows, TILE // 2), BF16))
    for i in range(bits):
        count = replicas >> (i + 1)
        scratch.append(pltpu.VMEM((PIECES + 1, 2, count, down_rows, piece // 2), BF16))
    scratch += [pltpu.SemaphoreType.DMA((3,))]
    scratch += [pltpu.SemaphoreType.DMA((1 + PIECES, 2, n))] * 2
    scratch += [pltpu.SemaphoreType.DMA((n,))] * 6
    scratch += [pltpu.SemaphoreType.DMA((chunks, bits, 2))] * 2
    scratch += [pltpu.SemaphoreType.DMA((PIECES + 1, bits, 2))] * 2
    scratch += [pltpu.SemaphoreType.DMA((2,))] * 2
    scratch += [pltpu.SemaphoreType.DMA((n,))] * 2
    input_grad, combine_grad, both, down = pl.pallas_call(
        functools.partial(layer_kernel, n, bits),
        out_shape=outs,
        in_specs=[VMEM] * 4 + [HBM] * 3,
        out_specs=[VMEM] * 4,
        scratch_shapes=scratch,
        compiler_params=pltpu.CompilerParams(
            collective_id=0, has_side_effects=True, vmem_limit_bytes=LIMIT
        ),
        name="layer",
    )(expert_ids.T, combine.T, tokens, cotangent, w_gate, w_up, w_down)
    return deliver(input_grad, combine_grad, both, down)


def solution(mesh):
    by_token = P(("dp", "expert"), None)
    by_expert = P("expert", None, None)
    by_row = P("expert", "dp", None)
    return jax.shard_map(
        shards,
        mesh=mesh,
        in_specs=(by_token,) * 4 + (by_expert,) * 3,
        out_specs=(by_token, by_token, by_row, by_row, by_row),
        check_vma=False,
    )
```

```python
import functools
import jax
import jax.numpy as jnp
from jax import lax
from jax.experimental import pallas as pl
from jax.experimental.pallas import tpu as pltpu
from jax.sharding import PartitionSpec as P

MESH = pl.DeviceIdType.MESH
VMEM = pl.BlockSpec(memory_space=pltpu.VMEM)
HBM = pl.BlockSpec(memory_space=pltpu.HBM)
LIMIT = 50 * 1024 * 1024
TILE = 256
WIDE = 512
PIECES = 4
LAST = (((1,), (1,)), ((), ()))
F32 = jnp.float32
BF16 = jnp.bfloat16


def remote(src, dst, send, recv, axis, target):
    return pltpu.make_async_remote_copy(
        src_ref=src,
        dst_ref=dst,
        send_sem=send,
        recv_sem=recv,
        device_id={axis: target},
        device_id_type=MESH,
    )


def span(index, size):
    return pl.ds(pl.multiple_of(index * size, size), size)


def loop(low, high, body, **options):
    def step(i, carry):
        body(i)
        return carry

    lax.fori_loop(low, high, step, 0, **options)


def layer_kernel(n, bits, *refs):
    routes, both_in, g_in, u_in, d_in = refs[:5]
    top = routes.shape[0] // 2
    ids, comb = routes.at[:top], routes.at[top:]
    x_in, dy_in = both_in.at[0], both_in.at[1]
    refs = (None, None) + refs
    in_grad, comb_grad, both_out, down_out = refs[7:11]
    x_all, dy_all, x_t, wg, wu, wd, slope, act_all = refs[11:19]
    h_all, h_t, pair_d, hid, rows_out, rows_got = refs[19:25]
    tables, comb_out, comb_got, h_guest, down_guest = refs[25:30]
    both_part, down_part = refs[30:32]
    both_got, down_got = refs[32 : 32 + bits], refs[32 + bits : 32 + 2 * bits]
    rest = refs[32 + 2 * bits :]
    load, a_send, a_recv, t_send, t_recv, r_send, r_recv, c_send, c_recv = rest[:9]
    b_send, b_recv, d_send, d_recv, f_send, f_recv, h_send, h_recv = rest[9:17]

    me = lax.axis_index("expert")
    rank = lax.axis_index("dp")
    replicas = 1 << bits
    half = replicas // 2
    rows = in_grad.shape[0]
    feature, width = wg.shape
    piece = feature // PIECES
    chunks = 2 * width // TILE
    both_rows, down_rows = both_out.shape[0], down_out.shape[0]
    bit = [lax.rem(rank // (1 << b), 2) for b in range(bits)]
    mate = [rank + (1 - 2 * bit[b]) * (1 << b) for b in range(bits)]
    orders = ([0] + list(range(1, bits)), [0] + list(range(bits - 1, 0, -1)))
    is_end = jnp.logical_or(me == 0, me == n - 1)
    is_mid = jnp.logical_not(is_end)

    loads = [
        pltpu.make_async_copy(src, dst, load.at[i])
        for i, (src, dst) in enumerate(
            (
                (g_in.at[0], wg),
                (u_in.at[0], wu),
                (d_in.at[0], wd),
            )
        )
    ]
    for item in loads:
        item.start()
    barrier = pltpu.get_barrier_semaphore()
    for k in range(1, n):
        pl.semaphore_signal(
            barrier, inc=1, device_id={"expert": lax.rem(me + k, n)}, device_id_type=MESH
        )
    for b in range(bits):
        pl.semaphore_signal(barrier, inc=1, device_id={"dp": mate[b]}, device_id_type=MESH)

    expert = lax.broadcasted_iota(jnp.int32, tables.shape[1:], 0).astype(F32)
    weight = jnp.where(expert == ids[0:1, :], comb[0:1, :], 0.0)
    for k in range(1, top):
        weight = weight + jnp.where(expert == ids[k : k + 1, :], comb[k : k + 1, :], 0.0)
    tables[me] = weight

    def view(p, block):
        if p is None:
            return x_all.at[span(block, rows)]
        return dy_all.at[span(block, rows), span(p, piece)]

    def index(p):
        return 0 if p is None else 1 + p

    def hop(p, side, s, own=False):
        step = 1 - 2 * side
        block = jnp.clip(me - step * s, 0, n - 1)
        slot = view(p, block)
        target = jnp.clip(me + step, 0, n - 1)
        i = index(p)
        src = slot
        if own:
            src = x_in if p is None else dy_in.at[:, span(p, piece)]
        return remote(src, slot, a_send.at[side, s], a_recv.at[i, block], "expert", target)

    def arrival(p, side, s):
        step = 1 - 2 * side
        block = jnp.clip(me - step * (s + 1), 0, n - 1)
        slot = view(p, block)
        return remote(slot, slot, a_send.at[side, s], a_recv.at[index(p), block], "expert", me)

    def hops(side, s):
        slot = x_all.at[pl.ds(0, 2 * rows)]
        return remote(slot, slot, a_send.at[side, s], a_recv.at[0, 0], "expert", me)

    def sends(side, s):
        if side == 0:
            return jnp.logical_and(me >= s, me + 1 < n)
        return jnp.logical_and(me + s < n, me >= 1)

    def passes(side):
        return jnp.where(side == 0, me + 1 < n, me >= 1)

    def table_copy(target):
        return remote(
            tables.at[me], tables.at[me], t_send.at[0], t_recv.at[me], "expert", target
        )

    def row_copy(target):
        return remote(
            rows_out.at[target],
            rows_got.at[me],
            r_send.at[target],
            r_recv.at[me],
            "expert",
            target,
        )

    def tile_copy(target, j):
        cols = span(j, WIDE)
        return remote(
            rows_out.at[target, :, cols],
            rows_got.at[me, :, cols],
            r_send.at[target],
            r_recv.at[me],
            "expert",
            target,
        )

    fold = n == 4
    ally = n - 1 - me
    near = jnp.where(2 * me < n, 0, n - 1)
    far = n - 1 - near

    shared = PIECES - 1 if fold else PIECES
    helper = jnp.where(me == 0, 1, n - 2)
    own_down = PIECES
    if fold:
        own_down = jnp.where(is_end, shared, PIECES + 1)

    def hidden_copy(b):
        cols = span(b, rows)
        return remote(
            h_t.at[:, cols], h_guest.at[:, cols], h_send.at[0], h_recv.at[0], "expert", helper
        )

    def guest_copy():
        return remote(
            down_guest,
            down_out.at[:, span(PIECES - 1, piece)],
            f_send.at[1],
            f_recv.at[1],
            "expert",
            near,
        )

    def fold_copy():
        return remote(
            rows_out.at[far], rows_got.at[ally], f_send.at[0], f_recv.at[0], "expert", ally
        )

    def folded():
        slot = rows_got.at[me]
        return remote(slot, slot, f_send.at[0], f_recv.at[0], "expert", me)

    def comb_copy(target):
        return remote(
            comb_out.at[target],
            comb_got.at[me],
            c_send.at[0],
            c_recv.at[0],
            "expert",
            target,
        )

    def few(ref, send, recv):
        slot = ref.at[pl.ds(0, n - 1)]
        return remote(slot, slot, send.at[0], recv.at[0], "expert", me)

    pl.semaphore_wait(barrier, n - 1 + bits)
    others = [lax.rem(me + k, n) for k in range(1, n)]
    for target in others:
        table_copy(target).start()
    for p in [None] + list(range(PIECES)):
        for side in range(2):
            ready = sends(side, 0)
            if p is not None and p > 0:
                ready = jnp.logical_and(ready, me == (0, n - 1)[side])

            @pl.when(ready)
            def _():
                hop(p, side, 0, True).start()

    x_all[span(me, rows), :] = x_in[...]
    dy_all[span(me, rows), :] = dy_in[...]
    for item in loads:
        item.wait()

    def coefficient(b):
        line = tables[b, pl.ds(me, 1), :]
        return jnp.broadcast_to(line, (128, rows)).T[:, 0:1]

    def forward(b):
        own = span(b, rows)
        coef = coefficient(b)

        def tile(j):
            cols = span(j, TILE)
            value = x_all[own, :]
            gate = jnp.dot(value, wg[:, cols], preferred_element_type=F32)
            up = jnp.dot(value, wu[:, cols], preferred_element_type=F32)
            sig = jax.nn.sigmoid(gate)
            act = gate * sig
            hidden = (act * up).astype(BF16)
            slope[own, cols] = up * (sig * (1.0 + gate * (1.0 - sig)))
            act_all[own, cols] = act
            h_all[own, cols] = hidden
            h_t[cols, own] = (coef * hidden.astype(F32)).T.astype(BF16)

        loop(0, width // TILE, tile)

        def turn(j):
            cols = span(j, TILE)
            x_t[cols, own] = x_all[own, cols].T

        if fold:

            @pl.when(is_end)
            def _():
                hidden_copy(b).start()

        loop(0, feature // TILE, turn)

    def gather_hidden(b, q, slot=0):
        cols = span(q, piece)
        hid[slot] += lax.dot_general(
            dy_all[span(b, rows), cols], wd[:, cols], LAST, preferred_element_type=F32
        )

    def slopes(b, slot=0):
        own = span(b, rows)
        coef = coefficient(b)

        def tile(j, total):
            cols = span(j, TILE)
            grad = hid[slot, :, cols]
            total = total + jnp.sum(h_all[own, cols].astype(F32) * grad, axis=1, keepdims=True)
            grad = coef * grad
            pair_d[own, cols] = (grad * slope[own, cols]).astype(BF16)
            pair_d[own, span(width // TILE + j, TILE)] = (grad * act_all[own, cols]).astype(BF16)
            return total

        total = lax.fori_loop(0, width // TILE, tile, jnp.zeros((rows, 1), F32))
        comb_out[b] = jnp.broadcast_to(total, (rows, 128)).T[:8]

    def input_tile(b, j):
        own = span(b, rows)
        cols = span(j, WIDE)
        value = lax.dot_general(pair_d[own, :width], wg[cols, :], LAST, preferred_element_type=F32)
        value = value + lax.dot_general(
            pair_d[own, width:], wu[cols, :], LAST, preferred_element_type=F32
        )
        rows_out[b, :, cols] = value.astype(BF16)

    def send_rows(b):
        row_copy(b).start()
        comb_copy(b).start()

    def first(d):
        return jnp.where(jnp.logical_or(d == 0, me >= d), 0, 1)

    def bound(d):
        return jnp.where(jnp.logical_and(d > 0, me + d < n), 2, 1)

    def source(side, d):
        return jnp.clip(me + d * (2 * side - 1), 0, n - 1)

    def by_end(side):
        return jnp.where(side == 0, me == n - 2, me == 1)

    def back(b, d):
        hid[0] = jnp.zeros(hid.shape[1:], F32)
        loop(0, PIECES, lambda q: gather_hidden(b, q))
        slopes(b)
        loop(0, feature // WIDE, functools.partial(input_tile, b))

        @pl.when(jnp.logical_and(is_end, d > 0))
        def _():
            send_rows(b)

    def distance(d):
        def take(side):
            @pl.when(d > 0)
            def _():
                arrival(None, side, d - 1).wait_recv()
                b = source(side, d)
                remote(
                    tables.at[b], tables.at[b], t_send.at[0], t_recv.at[b], "expert", me
                ).wait_recv()

                @pl.when(passes(side))
                def _():
                    hop(None, side, d).start()

                    @pl.when(d == 1)
                    def _():
                        for p in range(1, PIECES):
                            hop(p, side, 0, True).start()

        loop(first(d), bound(d), take)
        loop(first(d), bound(d), lambda side: forward(source(side, d)))
        e = jnp.maximum(d - 1, 0)

        def take_piece(i):
            q, side = i // 2, lax.rem(i, 2)
            here = jnp.logical_and(side >= first(e), side < bound(e))

            @pl.when(jnp.logical_and(here, e > 0))
            def _():
                arrival(q, side, e - 1).wait_recv()
                later = jnp.logical_and(by_end(side), e == n - 3)

                @pl.when(jnp.logical_and(passes(side), jnp.logical_not(later)))
                def _():
                    hop(q, side, e).start()

        @pl.when(jnp.logical_or(d == 0, jnp.logical_and(d > 1, d < n - 1)))
        def _():
            loop(0, 2 * PIECES, take_piece)
            loop(first(e), bound(e), lambda side: back(source(side, e), e))

    loop(0, n, distance)

    @pl.when(jnp.logical_or(me == 1, me == n - 2))
    def _():
        side = jnp.where(me == 1, 1, 0)

        def take(q):
            arrival(q, side, n - 3).wait_recv()
            hop(q, side, n - 3).start()
            hop(q, side, n - 2).start()

        loop(0, PIECES, take)
        back(source(side, n - 2), n - 2)

    if fold:

        @pl.when(is_mid)
        def _():
            fold_copy().start()
            send_rows(ally)

    else:
        for target in others:
            inner = jnp.logical_and(target > 0, target < n - 1)

            @pl.when(jnp.logical_and(is_mid, inner))
            def _():
                send_rows(target)

    def place_of(way, who):
        value = 0
        for i, b in enumerate(orders[way]):
            value = value + lax.rem(who // (1 << b), 2) * (1 << (bits - 1 - i))
        return value

    kinds = {
        "both": (both_part, both_got, b_send, b_recv),
        "down": (down_part, down_got, d_send, d_recv),
    }

    def base(way, i):
        value = 0
        for j in range(i):
            value = value + bit[orders[way][j]] * (replicas >> (j + 1))
        return value

    def stage(kind, c, way, i):
        part, got, send, recv = kinds[kind]
        b = orders[way][i]
        count = replicas >> (i + 1)
        start = base(way, i) + (1 - bit[b]) * count
        pick = slice(None) if i == 0 else way
        return remote(
            part.at[c, pick, pl.ds(start, count)],
            got[i].at[c, pick],
            send.at[c],
            recv.at[c, i],
            "dp",
            mate[b],
        )

    def staged(kind, c):
        part, _, send, recv = kinds[kind]
        slot = part.at[c, :, pl.ds(0, replicas - 1)]
        return remote(slot, slot, send.at[c], recv.at[c, 0], "dp", rank)

    def combine(kind, c, i):
        part, got, _, _ = kinds[kind]
        count = replicas >> (i + 1)
        recv = kinds[kind][3]
        slot = got[i].at[c]
        remote(slot, slot, kinds[kind][2].at[c], recv.at[c, i], "dp", rank).wait_recv()
        for way in range(2):
            start = base(way, i + 1)
            if i == bits - 1:
                total = part[c, way, start].astype(F32) + got[i][c, way, 0].astype(F32)
                if kind == "both":
                    both_out[:, span(2 * c + way, TILE // 2)] = total.astype(BF16)
                elif fold:

                    @pl.when(c < PIECES)
                    def _():
                        down_out[:, span(2 * c + way, piece // 2)] = total.astype(BF16)

                    @pl.when(c == PIECES)
                    def _():
                        down_guest[:, span(way, piece // 2)] = total.astype(BF16)

                else:
                    down_out[:, span(2 * c + way, piece // 2)] = total.astype(BF16)
                continue

            def add(k):
                total = part[c, way, start + k].astype(F32) + got[i][c, way, k].astype(F32)
                part[c, way, start + k] = total.astype(BF16)

            loop(0, count, add)
            stage(kind, c, way, i + 1).start()

    def spread(kind, c, who, value):
        part = kinds[kind][0]
        size = value.shape[1] // 2
        for way in range(2):
            half_value = value[:, way * size : (way + 1) * size]
            part[c, way, place_of(way, who)] = half_value.astype(BF16)

    def both_chunk(c):
        def place(side, j):
            who = 2 * j + side
            lines = span(who, both_rows)
            value = jnp.dot(x_t[lines, :], pair_d[:, span(c, TILE)], preferred_element_type=F32)
            spread("both", c, who, value)

        loop(0, half, functools.partial(place, 1 - bit[0]), unroll=2)
        stage("both", c, 0, 0).start()
        loop(0, half, functools.partial(place, bit[0]), unroll=2)

    def down_chunk(q, held=h_t):
        cols = span(min(q, PIECES - 1) if isinstance(q, int) else q, piece)
        group = 1 if down_rows % 16 == 0 else 2

        def place(side, j):
            who = 2 * j + side
            lines = span(who // group, group * down_rows)
            value = jnp.dot(held[lines, :], dy_all[:, cols], preferred_element_type=F32)
            for k in range(group):
                spread("down", q, who + k, value[k * down_rows : (k + 1) * down_rows])

        if group == 1:
            loop(0, half, functools.partial(place, 1 - bit[0]), unroll=2)
            stage("down", q, 0, 0).start()
            loop(0, half, functools.partial(place, bit[0]), unroll=2)
        else:
            loop(0, half, functools.partial(place, 0))
            stage("down", q, 0, 0).start()

    last = jnp.clip(n - 1 - me, 0, n - 1)
    prior = jnp.where(me == n - 1, 1, n - 2)
    last_side = jnp.where(me == n - 1, 0, 1)

    @pl.when(is_end)
    def _():
        hid[...] = jnp.zeros_like(hid)

    wide = feature // WIDE

    def last_tile(j):
        @pl.when(jnp.logical_and(is_end, j < 2 * wide))
        def _():
            b = jnp.where(j < wide, last, prior)
            tile = lax.rem(j, wide)
            input_tile(b, tile)
            tile_copy(b, tile).start()

            @pl.when(tile == wide - 1)
            def _():
                comb_copy(b).start()

    def early(q):
        @pl.when(is_end)
        def _():
            for slot, b in enumerate((prior, last)):
                arrival(q, last_side, n - 3 + slot).wait_recv()
                gather_hidden(b, q, slot)

        down_chunk(q)
        combine("down", q, 0)

        @pl.when(q > 0)
        def _():
            combine("down", q - 1, 1)

    loop(0, PIECES - 1, early)

    @pl.when(is_end)
    def _():
        for slot, b in enumerate((prior, last)):
            arrival(PIECES - 1, last_side, n - 3 + slot).wait_recv()
            gather_hidden(b, PIECES - 1, slot)
            slopes(b, slot)

    if fold:

        @pl.when(is_mid)
        def _():
            remote(h_guest, h_guest, h_send.at[0], h_recv.at[0], "expert", me).wait_recv()
            down_chunk(PIECES, h_guest)

    both_chunk(0)
    both_chunk(1)
    combine("both", 0, 0)
    combine("down", PIECES - 2, 1)
    last_tile(0)
    combine("both", 1, 0)

    def rest_down(i):
        if i == 0:
            down_chunk(PIECES - 1)
            if fold:
                combine("down", PIECES, 0)
        combine("down", PIECES - 1, i)
        if fold and i > 0:
            combine("down", PIECES, i)

    def when_owned(body):
        if fold:
            pl.when(is_mid)(body)
        else:
            body()

    when_owned(lambda: rest_down(0))
    last_tile(1)
    last_tile(2)

    def settle():
        for side in range(2):
            for s in range(n - 1):

                @pl.when(sends(side, s))
                def _():
                    hops(side, s).wait_send()

        if fold:

            @pl.when(is_mid)
            def _():
                folded().wait_recv()

                def add(j):
                    cols = span(j, TILE)
                    total = rows_out[near, :, cols].astype(F32) + rows_got[me, :, cols].astype(F32)
                    rows_out[near, :, cols] = total.astype(BF16)

                loop(0, feature // TILE, add)
                row_copy(near).start()
                comb_copy(near).start()
                comb_copy(far).start()

        else:
            for target in others:
                outer = jnp.logical_or(target == 0, target == n - 1)

                @pl.when(jnp.logical_and(is_mid, outer))
                def _():
                    send_rows(target)

    def late(c):
        both_chunk(c)
        for t in range(2):
            last_tile(2 * c - 1 + t)
        combine("both", c, 0)

        @pl.when(c == 3)
        def _():
            when_owned(lambda: rest_down(1))

        @pl.when(c == 2)
        def _():
            settle()

    loop(2, chunks, late)

    for i in range(1, bits - 1):
        if i > 1:
            loop(0, own_down, lambda q: combine("down", q, i))
        loop(0, chunks, lambda c: combine("both", c, i))

    loop(0, own_down, lambda q: combine("down", q, bits - 1))
    if fold:

        @pl.when(is_mid)
        def _():
            guest_copy().start()


    def takes_row(b):
        if not fold:
            return b >= 0
        return jnp.logical_or(is_mid, b != jnp.where(me == 0, n - 2, 1))

    def gives_row(target):
        if not fold:
            return target >= 0
        return jnp.logical_or(is_end, target != far)

    for b in others:

        @pl.when(takes_row(b))
        def _():
            remote(
                rows_got.at[b], rows_got.at[b], r_send.at[b], r_recv.at[b], "expert", me
            ).wait_recv()


    few(comb_got, c_send, c_recv).wait_recv()

    def total_rows(who):
        def tile(j):
            cols = span(j, TILE)
            total = rows_out[me, :, cols].astype(F32)
            for b in who:
                total = total + rows_got[b, :, cols].astype(F32)
            in_grad[:, cols] = total.astype(BF16)

        loop(0, feature // TILE, tile)

    if fold:

        @pl.when(is_end)
        def _():
            total_rows([n - 1 - me, jnp.where(me == 0, 1, n - 2)])

        @pl.when(is_mid)
        def _():
            total_rows(others)

    else:
        total_rows(others)

    picked = jnp.where(ids[...] == me.astype(F32), comb_out[me, 0:1, :], 0.0)
    for b in others:
        picked = picked + jnp.where(ids[...] == b.astype(F32), comb_got[b, 0:1, :], 0.0)
    comb_grad[...] = picked

    if fold:

        @pl.when(is_end)
        def _():
            slot = down_out.at[:, span(PIECES - 1, piece)]
            remote(slot, slot, f_send.at[1], f_recv.at[1], "expert", me).wait_recv()
            remote(h_t, h_t, h_send.at[0], h_recv.at[0], "expert", me).wait_send()

        @pl.when(is_mid)
        def _():
            guest_copy().wait_send()

    few(tables, t_send, t_recv).wait_send()
    few(comb_out, c_send, c_recv).wait_send()
    for target in others:

        @pl.when(gives_row(target))
        def _():
            row_copy(target).wait_send()

    if fold:

        @pl.when(is_mid)
        def _():
            fold_copy().wait_send()

    loop(0, own_down, lambda q: staged("down", q).wait_send())

    def finish(c):
        combine("both", c, bits - 1)
        staged("both", c).wait_send()

    loop(0, chunks, finish)


def deliver_kernel(rows, comb, both, down, *refs):
    outs, sems = refs[:-1], refs[-1]
    width = outs[2].shape[2]
    copies = []
    for src, dst in (
        (rows, outs[0]),
        (both.at[:, pl.ds(0, width)], outs[2].at[0]),
        (both.at[:, pl.ds(width, width)], outs[3].at[0]),
        (down, outs[4].at[0]),
        (comb, outs[1]),
    ):
        copies.append(pltpu.make_async_copy(src, dst, sems.at[len(copies)]))
        copies[-1].start()
    for copy in copies:
        copy.wait()


def deliver(rows, comb, both, down):
    width = both.shape[1] // 2
    outs = [
        jax.ShapeDtypeStruct(rows.shape, BF16),
        jax.ShapeDtypeStruct(comb.shape, F32),
        jax.ShapeDtypeStruct((1, both.shape[0], width), BF16),
        jax.ShapeDtypeStruct((1, both.shape[0], width), BF16),
        jax.ShapeDtypeStruct((1,) + down.shape, BF16),
    ]
    input_grad, combine_grad, gate_grad, up_grad, down_grad = pl.pallas_call(
        deliver_kernel,
        out_shape=outs,
        in_specs=[VMEM] * 4,
        out_specs=[HBM] * 5,
        scratch_shapes=[pltpu.SemaphoreType.DMA((5,))],
        compiler_params=pltpu.CompilerParams(vmem_limit_bytes=8 * 1024 * 1024),
        name="deliver",
    )(rows, comb, both, down)
    return (input_grad, combine_grad.T, gate_grad, up_grad, down_grad)


def shards(tokens, cotangent, expert_ids, combine, w_gate, w_up, w_down):
    n = lax.axis_size("expert")
    replicas = lax.axis_size("dp")
    bits = replicas.bit_length() - 1
    rows, top = expert_ids.shape
    feature = tokens.shape[1]
    width = w_gate.shape[2]
    everyone = n * rows
    chunks = 2 * width // TILE
    piece = feature // PIECES
    both_rows, down_rows = feature // replicas, width // replicas
    table = -(-n // 8) * 8
    outs = [
        jax.ShapeDtypeStruct((rows, feature), BF16),
        jax.ShapeDtypeStruct((top, rows), F32),
        jax.ShapeDtypeStruct((both_rows, 2 * width), BF16),
        jax.ShapeDtypeStruct((down_rows, feature), BF16),
    ]
    scratch = [
        pltpu.VMEM((everyone, feature), BF16),
        pltpu.VMEM((everyone, feature), BF16),
        pltpu.VMEM((feature, everyone), BF16),
        pltpu.VMEM((feature, width), BF16),
        pltpu.VMEM((feature, width), BF16),
        pltpu.VMEM((width, feature), BF16),
        pltpu.VMEM((everyone, width), F32),
        pltpu.VMEM((everyone, width), F32),
        pltpu.VMEM((everyone, width), BF16),
        pltpu.VMEM((width, everyone), BF16),
        pltpu.VMEM((everyone, 2 * width), BF16),
        pltpu.VMEM((2, rows, width), F32),
        pltpu.VMEM((n, rows, feature), BF16),
        pltpu.VMEM((n, rows, feature), BF16),
        pltpu.VMEM((n, table, rows), F32),
        pltpu.VMEM((n, 8, rows), F32),
        pltpu.VMEM((n, 8, rows), F32),
        pltpu.VMEM((width, everyone), BF16),
        pltpu.VMEM((down_rows, piece), BF16),
        pltpu.VMEM((chunks, 2, replicas, both_rows, TILE // 2), BF16),
        pltpu.VMEM((PIECES + 1, 2, replicas, down_rows, piece // 2), BF16),
    ]
    for i in range(bits):
        count = replicas >> (i + 1)
        scratch.append(pltpu.VMEM((chunks, 2, count, both_rows, TILE // 2), BF16))
    for i in range(bits):
        count = replicas >> (i + 1)
        scratch.append(pltpu.VMEM((PIECES + 1, 2, count, down_rows, piece // 2), BF16))
    scratch += [pltpu.SemaphoreType.DMA((3,))]
    for shape in ((2, n - 1), (1 + PIECES, n), (1,), (n,), (n,), (n,), (1,), (1,)):
        scratch.append(pltpu.SemaphoreType.DMA(shape))
    for count in (chunks, PIECES + 1):
        scratch += [pltpu.SemaphoreType.DMA((count,)), pltpu.SemaphoreType.DMA((count, bits))]
    scratch += [pltpu.SemaphoreType.DMA((2,))] * 2
    scratch += [pltpu.SemaphoreType.DMA((1,))] * 2
    routes = jnp.concatenate([expert_ids.T.astype(F32), combine.T])
    input_grad, combine_grad, both, down = pl.pallas_call(
        functools.partial(layer_kernel, n, bits),
        out_shape=outs,
        in_specs=[VMEM] * 2 + [HBM] * 3,
        out_specs=[VMEM] * 4,
        scratch_shapes=scratch,
        compiler_params=pltpu.CompilerParams(
            collective_id=0, has_side_effects=True, vmem_limit_bytes=LIMIT
        ),
        name="layer",
    )(routes, jnp.stack([tokens, cotangent]), w_gate, w_up, w_down)
    return deliver(input_grad, combine_grad, both, down)


def solution(mesh):
    by_token = P(("dp", "expert"), None)
    by_expert = P("expert", None, None)
    by_row = P("expert", "dp", None)
    return jax.shard_map(
        shards,
        mesh=mesh,
        in_specs=(by_token,) * 4 + (by_expert,) * 3,
        out_specs=(by_token, by_token, by_row, by_row, by_row),
        check_vma=False,
    )
```

```python
import functools
import jax
import jax.numpy as jnp
from jax import lax
from jax.experimental import pallas as pl
from jax.experimental.pallas import tpu as pltpu
from jax.sharding import PartitionSpec as P

MESH = pl.DeviceIdType.MESH
VMEM = pl.BlockSpec(memory_space=pltpu.VMEM)
HBM = pl.BlockSpec(memory_space=pltpu.HBM)
LIMIT = 50 * 1024 * 1024
TILE = 256
WIDE = 512
PIECES = 4
LAST = (((1,), (1,)), ((), ()))
F32 = jnp.float32
BF16 = jnp.bfloat16


def remote(src, dst, send, recv, axis, target):
    return pltpu.make_async_remote_copy(
        src_ref=src,
        dst_ref=dst,
        send_sem=send,
        recv_sem=recv,
        device_id={axis: target},
        device_id_type=MESH,
    )


def span(index, size):
    return pl.ds(pl.multiple_of(index * size, size), size)


def loop(low, high, body, **options):
    def step(i, carry):
        body(i)
        return carry

    lax.fori_loop(low, high, step, 0, **options)


def layer_kernel(n, bits, *refs):
    routes, both_in, g_in, u_in, d_in = refs[:5]
    top = routes.shape[1]
    x_in, dy_in = both_in.at[0], both_in.at[1]
    refs = (None, None) + refs
    in_grad, comb_grad, both_out, down_out = refs[7:11]
    x_all, dy_all, x_t, wg, wu, wd, slope, act_all = refs[11:19]
    h_all, h_t, pair_d, hid, rows_out, rows_got = refs[19:25]
    tables, comb_out, comb_got, h_guest, down_guest = refs[25:30]
    both_part, down_part = refs[30:32]
    both_got, down_got = refs[32 : 32 + bits], refs[32 + bits : 32 + 2 * bits]
    rest = refs[32 + 2 * bits :]
    load, a_send, a_recv, t_send, t_recv, r_send, r_recv, c_send, c_recv = rest[:9]
    b_send, b_recv, d_send, d_recv, f_send, f_recv, h_send, h_recv = rest[9:17]

    me = lax.axis_index("expert")
    rank = lax.axis_index("dp")
    replicas = 1 << bits
    half = replicas // 2
    rows = in_grad.shape[0]
    feature, width = wg.shape
    piece = feature // PIECES
    chunks = 2 * width // TILE
    both_rows, down_rows = both_out.shape[0], down_out.shape[0]
    bit = [lax.rem(rank // (1 << b), 2) for b in range(bits)]
    mate = [rank + (1 - 2 * bit[b]) * (1 << b) for b in range(bits)]
    orders = ([0] + list(range(1, bits)), [0] + list(range(bits - 1, 0, -1)))
    is_end = jnp.logical_or(me == 0, me == n - 1)
    is_mid = jnp.logical_not(is_end)

    loads = [
        pltpu.make_async_copy(src, dst, load.at[i])
        for i, (src, dst) in enumerate(
            (
                (g_in.at[0], wg),
                (u_in.at[0], wu),
                (d_in.at[0], wd),
            )
        )
    ]
    for item in loads:
        item.start()
    barrier = pltpu.get_barrier_semaphore()
    for k in range(1, n):
        pl.semaphore_signal(
            barrier, inc=1, device_id={"expert": lax.rem(me + k, n)}, device_id_type=MESH
        )
    for b in range(bits):
        pl.semaphore_signal(barrier, inc=1, device_id={"dp": mate[b]}, device_id_type=MESH)

    weight = routes[1, 0]
    for k in range(1, top):
        weight = weight + routes[1, k]
    tables[me] = weight

    def view(p, block):
        if p is None:
            return x_all.at[span(block, rows)]
        return dy_all.at[span(block, rows), span(p, piece)]

    def index(p):
        return 0 if p is None else 1 + p

    def hop(p, side, s, own=False):
        step = 1 - 2 * side
        block = jnp.clip(me - step * s, 0, n - 1)
        slot = view(p, block)
        target = jnp.clip(me + step, 0, n - 1)
        i = index(p)
        src = slot
        if own:
            src = x_in if p is None else dy_in.at[:, span(p, piece)]
        return remote(src, slot, a_send.at[side, s], a_recv.at[i, block], "expert", target)

    def arrival(p, side, s):
        step = 1 - 2 * side
        block = jnp.clip(me - step * (s + 1), 0, n - 1)
        slot = view(p, block)
        return remote(slot, slot, a_send.at[side, s], a_recv.at[index(p), block], "expert", me)

    def hops(side, s):
        slot = x_all.at[pl.ds(0, 2 * rows)]
        return remote(slot, slot, a_send.at[side, s], a_recv.at[0, 0], "expert", me)

    def sends(side, s):
        if side == 0:
            return jnp.logical_and(me >= s, me + 1 < n)
        return jnp.logical_and(me + s < n, me >= 1)

    def passes(side):
        return jnp.where(side == 0, me + 1 < n, me >= 1)

    def table_copy(target):
        return remote(
            tables.at[me], tables.at[me], t_send.at[0], t_recv.at[me], "expert", target
        )

    def row_copy(target):
        return remote(
            rows_out.at[target],
            rows_got.at[me],
            r_send.at[target],
            r_recv.at[me],
            "expert",
            target,
        )

    def tile_copy(target, j):
        cols = span(j, WIDE)
        return remote(
            rows_out.at[target, :, cols],
            rows_got.at[me, :, cols],
            r_send.at[target],
            r_recv.at[me],
            "expert",
            target,
        )

    fold = n == 4
    ally = n - 1 - me
    near = jnp.where(2 * me < n, 0, n - 1)
    far = n - 1 - near

    shared = PIECES - 1 if fold else PIECES
    helper = jnp.where(me == 0, 1, n - 2)
    own_down = PIECES
    if fold:
        own_down = jnp.where(is_end, shared, PIECES + 1)

    def hidden_copy(b):
        cols = span(b, rows)
        return remote(
            h_t.at[:, cols], h_guest.at[:, cols], h_send.at[0], h_recv.at[0], "expert", helper
        )

    def guest_copy():
        return remote(
            down_guest,
            down_out.at[:, span(PIECES - 1, piece)],
            f_send.at[1],
            f_recv.at[1],
            "expert",
            near,
        )

    def fold_copy():
        return remote(
            rows_out.at[far], rows_got.at[ally], f_send.at[0], f_recv.at[0], "expert", ally
        )

    def folded():
        slot = rows_got.at[me]
        return remote(slot, slot, f_send.at[0], f_recv.at[0], "expert", me)

    def comb_copy(target):
        return remote(
            comb_out.at[target],
            comb_got.at[me],
            c_send.at[0],
            c_recv.at[0],
            "expert",
            target,
        )

    def few(ref, send, recv):
        slot = ref.at[pl.ds(0, n - 1)]
        return remote(slot, slot, send.at[0], recv.at[0], "expert", me)

    pl.semaphore_wait(barrier, n - 1 + bits)
    others = [lax.rem(me + k, n) for k in range(1, n)]
    for target in others:
        table_copy(target).start()
    for p in [None] + list(range(PIECES)):
        for side in range(2):
            ready = sends(side, 0)
            if p is not None and p > 0:
                ready = jnp.logical_and(ready, me == (0, n - 1)[side])

            @pl.when(ready)
            def _():
                hop(p, side, 0, True).start()

    x_all[span(me, rows), :] = x_in[...]
    dy_all[span(me, rows), :] = dy_in[...]
    for item in loads:
        item.wait()

    def coefficient(b):
        line = tables[b, pl.ds(me, 1), :]
        return jnp.broadcast_to(line, (128, rows)).T[:, 0:1]

    def forward(b):
        own = span(b, rows)
        coef = coefficient(b)

        def tile(j):
            cols = span(j, TILE)
            value = x_all[own, :]
            gate = jnp.dot(value, wg[:, cols], preferred_element_type=F32)
            up = jnp.dot(value, wu[:, cols], preferred_element_type=F32)
            sig = jax.nn.sigmoid(gate)
            act = gate * sig
            hidden = (act * up).astype(BF16)
            slope[own, cols] = up * (sig * (1.0 + gate * (1.0 - sig)))
            act_all[own, cols] = act
            h_all[own, cols] = hidden
            h_t[cols, own] = (coef * hidden.astype(F32)).T.astype(BF16)

        loop(0, width // TILE, tile, unroll=True)

        def turn(j):
            cols = span(j, TILE)
            x_t[cols, own] = x_all[own, cols].T

        if fold:

            @pl.when(is_end)
            def _():
                hidden_copy(b).start()

        loop(0, feature // TILE, turn)

    def gather_hidden(b, q, slot=0):
        cols = span(q, piece)
        hid[slot] += lax.dot_general(
            dy_all[span(b, rows), cols], wd[:, cols], LAST, preferred_element_type=F32
        )

    def slopes(b, slot=0):
        own = span(b, rows)
        coef = coefficient(b)

        def tile(j, total):
            cols = span(j, TILE)
            grad = hid[slot, :, cols]
            total = total + jnp.sum(h_all[own, cols].astype(F32) * grad, axis=1, keepdims=True)
            grad = coef * grad
            pair_d[own, cols] = (grad * slope[own, cols]).astype(BF16)
            pair_d[own, span(width // TILE + j, TILE)] = (grad * act_all[own, cols]).astype(BF16)
            return total

        total = lax.fori_loop(0, width // TILE, tile, jnp.zeros((rows, 1), F32), unroll=True)
        comb_out[b] = jnp.broadcast_to(total, (rows, 128)).T[:8]

    def input_tile(b, j):
        own = span(b, rows)
        cols = span(j, WIDE)
        value = lax.dot_general(pair_d[own, :width], wg[cols, :], LAST, preferred_element_type=F32)
        value = value + lax.dot_general(
            pair_d[own, width:], wu[cols, :], LAST, preferred_element_type=F32
        )
        rows_out[b, :, cols] = value.astype(BF16)

    def send_rows(b):
        row_copy(b).start()
        comb_copy(b).start()

    def first(d):
        return jnp.where(jnp.logical_or(d == 0, me >= d), 0, 1)

    def bound(d):
        return jnp.where(jnp.logical_and(d > 0, me + d < n), 2, 1)

    def source(side, d):
        return jnp.clip(me + d * (2 * side - 1), 0, n - 1)

    def by_end(side):
        return jnp.where(side == 0, me == n - 2, me == 1)

    def back(b, d):
        hid[0] = jnp.zeros(hid.shape[1:], F32)
        loop(0, PIECES, lambda q: gather_hidden(b, q))
        slopes(b)
        loop(0, feature // WIDE, functools.partial(input_tile, b))

        @pl.when(jnp.logical_and(is_end, d > 0))
        def _():
            send_rows(b)

    def distance(d):
        def take(side):
            @pl.when(d > 0)
            def _():
                arrival(None, side, d - 1).wait_recv()
                b = source(side, d)
                remote(
                    tables.at[b], tables.at[b], t_send.at[0], t_recv.at[b], "expert", me
                ).wait_recv()

                @pl.when(passes(side))
                def _():
                    hop(None, side, d).start()

                    @pl.when(d == 1)
                    def _():
                        for p in range(1, PIECES):
                            hop(p, side, 0, True).start()

        loop(first(d), bound(d), take)
        loop(first(d), bound(d), lambda side: forward(source(side, d)))
        e = jnp.maximum(d - 1, 0)

        def take_piece(i):
            q, side = i // 2, lax.rem(i, 2)
            here = jnp.logical_and(side >= first(e), side < bound(e))

            @pl.when(jnp.logical_and(here, e > 0))
            def _():
                arrival(q, side, e - 1).wait_recv()
                later = jnp.logical_and(by_end(side), e == n - 3)

                @pl.when(jnp.logical_and(passes(side), jnp.logical_not(later)))
                def _():
                    hop(q, side, e).start()

        @pl.when(jnp.logical_or(d == 0, jnp.logical_and(d > 1, d < n - 1)))
        def _():
            loop(0, 2 * PIECES, take_piece)
            loop(first(e), bound(e), lambda side: back(source(side, e), e))

    loop(0, n, distance)

    @pl.when(jnp.logical_or(me == 1, me == n - 2))
    def _():
        side = jnp.where(me == 1, 1, 0)

        def take(q):
            arrival(q, side, n - 3).wait_recv()
            hop(q, side, n - 3).start()
            hop(q, side, n - 2).start()

        loop(0, PIECES, take)
        back(source(side, n - 2), n - 2)

    if fold:

        @pl.when(is_mid)
        def _():
            fold_copy().start()
            send_rows(ally)

    else:
        for target in others:
            inner = jnp.logical_and(target > 0, target < n - 1)

            @pl.when(jnp.logical_and(is_mid, inner))
            def _():
                send_rows(target)

    def place_of(way, who):
        value = 0
        for i, b in enumerate(orders[way]):
            value = value + lax.rem(who // (1 << b), 2) * (1 << (bits - 1 - i))
        return value

    kinds = {
        "both": (both_part, both_got, b_send, b_recv),
        "down": (down_part, down_got, d_send, d_recv),
    }

    def base(way, i):
        value = 0
        for j in range(i):
            value = value + bit[orders[way][j]] * (replicas >> (j + 1))
        return value

    def stage(kind, c, way, i):
        part, got, send, recv = kinds[kind]
        b = orders[way][i]
        count = replicas >> (i + 1)
        start = base(way, i) + (1 - bit[b]) * count
        pick = slice(None) if i == 0 else way
        return remote(
            part.at[c, pick, pl.ds(start, count)],
            got[i].at[c, pick],
            send.at[c],
            recv.at[c, i],
            "dp",
            mate[b],
        )

    def staged(kind, c):
        part, _, send, recv = kinds[kind]
        slot = part.at[c, :, pl.ds(0, replicas - 1)]
        return remote(slot, slot, send.at[c], recv.at[c, 0], "dp", rank)

    def combine(kind, c, i):
        part, got, _, _ = kinds[kind]
        count = replicas >> (i + 1)
        recv = kinds[kind][3]
        slot = got[i].at[c]
        remote(slot, slot, kinds[kind][2].at[c], recv.at[c, i], "dp", rank).wait_recv()
        for way in range(2):
            start = base(way, i + 1)
            if i == bits - 1:
                total = part[c, way, start].astype(F32) + got[i][c, way, 0].astype(F32)
                if kind == "both":
                    both_out[:, span(2 * c + way, TILE // 2)] = total.astype(BF16)
                elif fold:

                    @pl.when(c < PIECES)
                    def _():
                        down_out[:, span(2 * c + way, piece // 2)] = total.astype(BF16)

                    @pl.when(c == PIECES)
                    def _():
                        down_guest[:, span(way, piece // 2)] = total.astype(BF16)

                else:
                    down_out[:, span(2 * c + way, piece // 2)] = total.astype(BF16)
                continue

            def add(k):
                total = part[c, way, start + k].astype(F32) + got[i][c, way, k].astype(F32)
                part[c, way, start + k] = total.astype(BF16)

            loop(0, count, add)
            stage(kind, c, way, i + 1).start()

    def spread(kind, c, who, value):
        part = kinds[kind][0]
        size = value.shape[1] // 2
        for way in range(2):
            half_value = value[:, way * size : (way + 1) * size]
            part[c, way, place_of(way, who)] = half_value.astype(BF16)

    def both_chunk(c):
        def place(side, j):
            who = 2 * j + side
            lines = span(who, both_rows)
            value = jnp.dot(x_t[lines, :], pair_d[:, span(c, TILE)], preferred_element_type=F32)
            spread("both", c, who, value)

        loop(0, half, functools.partial(place, 1 - bit[0]), unroll=2)
        stage("both", c, 0, 0).start()
        loop(0, half, functools.partial(place, bit[0]), unroll=2)

    def down_chunk(q, held=h_t):
        cols = span(min(q, PIECES - 1) if isinstance(q, int) else q, piece)
        group = 1 if down_rows % 16 == 0 else 2

        def place(side, j):
            who = 2 * j + side
            lines = span(who // group, group * down_rows)
            value = jnp.dot(held[lines, :], dy_all[:, cols], preferred_element_type=F32)
            for k in range(group):
                spread("down", q, who + k, value[k * down_rows : (k + 1) * down_rows])

        if group == 1:
            loop(0, half, functools.partial(place, 1 - bit[0]), unroll=2)
            stage("down", q, 0, 0).start()
            loop(0, half, functools.partial(place, bit[0]), unroll=2)
        else:
            loop(0, half, functools.partial(place, 0))
            stage("down", q, 0, 0).start()

    last = jnp.clip(n - 1 - me, 0, n - 1)
    prior = jnp.where(me == n - 1, 1, n - 2)
    last_side = jnp.where(me == n - 1, 0, 1)

    @pl.when(is_end)
    def _():
        hid[...] = jnp.zeros_like(hid)

    wide = feature // WIDE

    def last_tile(j):
        @pl.when(jnp.logical_and(is_end, j < 2 * wide))
        def _():
            b = jnp.where(j < wide, last, prior)
            tile = lax.rem(j, wide)
            input_tile(b, tile)
            tile_copy(b, tile).start()

            @pl.when(tile == wide - 1)
            def _():
                comb_copy(b).start()

    def early(q):
        @pl.when(is_end)
        def _():
            for slot, b in enumerate((prior, last)):
                arrival(q, last_side, n - 3 + slot).wait_recv()
                gather_hidden(b, q, slot)

        down_chunk(q)
        combine("down", q, 0)

        @pl.when(q > 0)
        def _():
            combine("down", q - 1, 1)

    loop(0, PIECES - 1, early)

    @pl.when(is_end)
    def _():
        for slot, b in enumerate((prior, last)):
            arrival(PIECES - 1, last_side, n - 3 + slot).wait_recv()
            gather_hidden(b, PIECES - 1, slot)
            slopes(b, slot)

    if fold:

        @pl.when(is_mid)
        def _():
            remote(h_guest, h_guest, h_send.at[0], h_recv.at[0], "expert", me).wait_recv()
            down_chunk(PIECES, h_guest)

    both_chunk(0)
    both_chunk(1)
    combine("both", 0, 0)
    combine("down", PIECES - 2, 1)
    last_tile(0)
    combine("both", 1, 0)

    def rest_down(i):
        if i == 0:
            down_chunk(PIECES - 1)
            if fold:
                combine("down", PIECES, 0)
        combine("down", PIECES - 1, i)
        if fold and i > 0:
            combine("down", PIECES, i)

    def when_owned(body):
        if fold:
            pl.when(is_mid)(body)
        else:
            body()

    when_owned(lambda: rest_down(0))
    last_tile(1)
    last_tile(2)

    def settle():
        for side in range(2):
            for s in range(n - 1):

                @pl.when(sends(side, s))
                def _():
                    hops(side, s).wait_send()

        if fold:

            @pl.when(is_mid)
            def _():
                folded().wait_recv()

                def add(j):
                    cols = span(j, TILE)
                    total = rows_out[near, :, cols].astype(F32) + rows_got[me, :, cols].astype(F32)
                    rows_out[near, :, cols] = total.astype(BF16)

                loop(0, feature // TILE, add)
                row_copy(near).start()
                comb_copy(near).start()
                comb_copy(far).start()

        else:
            for target in others:
                outer = jnp.logical_or(target == 0, target == n - 1)

                @pl.when(jnp.logical_and(is_mid, outer))
                def _():
                    send_rows(target)

    def late(c):
        both_chunk(c)
        for t in range(2):
            last_tile(2 * c - 1 + t)
        combine("both", c, 0)

        @pl.when(c == 3)
        def _():
            when_owned(lambda: rest_down(1))

        @pl.when(c == 2)
        def _():
            settle()

    loop(2, chunks, late)

    for i in range(1, bits - 1):
        if i > 1:
            loop(0, own_down, lambda q: combine("down", q, i))
        loop(0, chunks, lambda c: combine("both", c, i))

    loop(0, own_down, lambda q: combine("down", q, bits - 1))
    if fold:

        @pl.when(is_mid)
        def _():
            guest_copy().start()


    def takes_row(b):
        if not fold:
            return b >= 0
        return jnp.logical_or(is_mid, b != jnp.where(me == 0, n - 2, 1))

    def gives_row(target):
        if not fold:
            return target >= 0
        return jnp.logical_or(is_end, target != far)

    for b in others:

        @pl.when(takes_row(b))
        def _():
            remote(
                rows_got.at[b], rows_got.at[b], r_send.at[b], r_recv.at[b], "expert", me
            ).wait_recv()


    few(comb_got, c_send, c_recv).wait_recv()

    def total_rows(who):
        def tile(j):
            cols = span(j, TILE)
            total = rows_out[me, :, cols].astype(F32)
            for b in who:
                total = total + rows_got[b, :, cols].astype(F32)
            in_grad[:, cols] = total.astype(BF16)

        loop(0, feature // TILE, tile)

    if fold:

        @pl.when(is_end)
        def _():
            total_rows([n - 1 - me, jnp.where(me == 0, 1, n - 2)])

        @pl.when(is_mid)
        def _():
            total_rows(others)

    else:
        total_rows(others)

    for k in range(top):

        def pick(b, line):
            return jnp.where(routes[0, k, pl.ds(b, 1), :] > 0.5, line, 0.0)

        picked = pick(me, comb_out[me, 0:1, :])
        for b in others:
            picked = picked + pick(b, comb_got[b, 0:1, :])
        comb_grad[k : k + 1, :] = picked

    if fold:

        @pl.when(is_end)
        def _():
            slot = down_out.at[:, span(PIECES - 1, piece)]
            remote(slot, slot, f_send.at[1], f_recv.at[1], "expert", me).wait_recv()
            remote(h_t, h_t, h_send.at[0], h_recv.at[0], "expert", me).wait_send()

        @pl.when(is_mid)
        def _():
            guest_copy().wait_send()

    few(tables, t_send, t_recv).wait_send()
    few(comb_out, c_send, c_recv).wait_send()
    for target in others:

        @pl.when(gives_row(target))
        def _():
            row_copy(target).wait_send()

    if fold:

        @pl.when(is_mid)
        def _():
            fold_copy().wait_send()

    loop(0, own_down, lambda q: staged("down", q).wait_send())

    def finish(c):
        combine("both", c, bits - 1)
        staged("both", c).wait_send()

    loop(0, chunks, finish)


def deliver_kernel(rows, comb, both, down, *refs):
    outs, sems = refs[:-1], refs[-1]
    width = outs[2].shape[2]
    copies = []
    for src, dst in (
        (rows, outs[0]),
        (both.at[:, pl.ds(0, width)], outs[2].at[0]),
        (both.at[:, pl.ds(width, width)], outs[3].at[0]),
        (down, outs[4].at[0]),
        (comb, outs[1]),
    ):
        copies.append(pltpu.make_async_copy(src, dst, sems.at[len(copies)]))
        copies[-1].start()
    for copy in copies:
        copy.wait()


def deliver(rows, comb, both, down):
    width = both.shape[1] // 2
    outs = [
        jax.ShapeDtypeStruct(rows.shape, BF16),
        jax.ShapeDtypeStruct(comb.shape, F32),
        jax.ShapeDtypeStruct((1, both.shape[0], width), BF16),
        jax.ShapeDtypeStruct((1, both.shape[0], width), BF16),
        jax.ShapeDtypeStruct((1,) + down.shape, BF16),
    ]
    input_grad, combine_grad, gate_grad, up_grad, down_grad = pl.pallas_call(
        deliver_kernel,
        out_shape=outs,
        in_specs=[VMEM] * 4,
        out_specs=[HBM] * 5,
        scratch_shapes=[pltpu.SemaphoreType.DMA((5,))],
        compiler_params=pltpu.CompilerParams(vmem_limit_bytes=8 * 1024 * 1024),
        name="deliver",
    )(rows, comb, both, down)
    return (input_grad, combine_grad.T, gate_grad, up_grad, down_grad)


def shards(tokens, cotangent, expert_ids, combine, w_gate, w_up, w_down):
    n = lax.axis_size("expert")
    replicas = lax.axis_size("dp")
    bits = replicas.bit_length() - 1
    rows, top = expert_ids.shape
    feature = tokens.shape[1]
    width = w_gate.shape[2]
    everyone = n * rows
    chunks = 2 * width // TILE
    piece = feature // PIECES
    both_rows, down_rows = feature // replicas, width // replicas
    table = -(-n // 8) * 8
    outs = [
        jax.ShapeDtypeStruct((rows, feature), BF16),
        jax.ShapeDtypeStruct((top, rows), F32),
        jax.ShapeDtypeStruct((both_rows, 2 * width), BF16),
        jax.ShapeDtypeStruct((down_rows, feature), BF16),
    ]
    scratch = [
        pltpu.VMEM((everyone, feature), BF16),
        pltpu.VMEM((everyone, feature), BF16),
        pltpu.VMEM((feature, everyone), BF16),
        pltpu.VMEM((feature, width), BF16),
        pltpu.VMEM((feature, width), BF16),
        pltpu.VMEM((width, feature), BF16),
        pltpu.VMEM((everyone, width), F32),
        pltpu.VMEM((everyone, width), F32),
        pltpu.VMEM((everyone, width), BF16),
        pltpu.VMEM((width, everyone), BF16),
        pltpu.VMEM((everyone, 2 * width), BF16),
        pltpu.VMEM((2, rows, width), F32),
        pltpu.VMEM((n, rows, feature), BF16),
        pltpu.VMEM((n, rows, feature), BF16),
        pltpu.VMEM((n, table, rows), F32),
        pltpu.VMEM((n, 8, rows), F32),
        pltpu.VMEM((n, 8, rows), F32),
        pltpu.VMEM((width, everyone), BF16),
        pltpu.VMEM((down_rows, piece), BF16),
        pltpu.VMEM((chunks, 2, replicas, both_rows, TILE // 2), BF16),
        pltpu.VMEM((PIECES + 1, 2, replicas, down_rows, piece // 2), BF16),
    ]
    for i in range(bits):
        count = replicas >> (i + 1)
        scratch.append(pltpu.VMEM((chunks, 2, count, both_rows, TILE // 2), BF16))
    for i in range(bits):
        count = replicas >> (i + 1)
        scratch.append(pltpu.VMEM((PIECES + 1, 2, count, down_rows, piece // 2), BF16))
    scratch += [pltpu.SemaphoreType.DMA((3,))]
    for shape in ((2, n - 1), (1 + PIECES, n), (1,), (n,), (n,), (n,), (1,), (1,)):
        scratch.append(pltpu.SemaphoreType.DMA(shape))
    for count in (chunks, PIECES + 1):
        scratch += [pltpu.SemaphoreType.DMA((count,)), pltpu.SemaphoreType.DMA((count, bits))]
    scratch += [pltpu.SemaphoreType.DMA((2,))] * 2
    scratch += [pltpu.SemaphoreType.DMA((1,))] * 2
    names = lax.broadcasted_iota(jnp.int32, (2, top, table, rows), 2)
    kind = lax.broadcasted_iota(jnp.int32, (2, top, table, rows), 0)
    value = jnp.where(kind == 0, 1.0, combine.T[None, :, None, :])
    routes = jnp.where(names == expert_ids.T[None, :, None, :], value, 0.0)
    input_grad, combine_grad, both, down = pl.pallas_call(
        functools.partial(layer_kernel, n, bits),
        out_shape=outs,
        in_specs=[VMEM] * 2 + [HBM] * 3,
        out_specs=[VMEM] * 4,
        scratch_shapes=scratch,
        compiler_params=pltpu.CompilerParams(
            collective_id=0, has_side_effects=True, vmem_limit_bytes=LIMIT
        ),
        name="layer",
    )(routes, jnp.stack([tokens, cotangent]), w_gate, w_up, w_down)
    return deliver(input_grad, combine_grad, both, down)


def solution(mesh):
    by_token = P(("dp", "expert"), None)
    by_expert = P("expert", None, None)
    by_row = P("expert", "dp", None)
    return jax.shard_map(
        shards,
        mesh=mesh,
        in_specs=(by_token,) * 4 + (by_expert,) * 3,
        out_specs=(by_token, by_token, by_row, by_row, by_row),
        check_vma=False,
    )
```

```python
import functools
import jax
import jax.numpy as jnp
from jax import lax
from jax.experimental import pallas as pl
from jax.experimental.pallas import tpu as pltpu
from jax.sharding import PartitionSpec as P

MESH = pl.DeviceIdType.MESH
VMEM = pl.BlockSpec(memory_space=pltpu.VMEM)
HBM = pl.BlockSpec(memory_space=pltpu.HBM)
LIMIT = 50 * 1024 * 1024
TILE = 256
WIDE = 512
PIECES = 4
LAST = (((1,), (1,)), ((), ()))
F32 = jnp.float32
BF16 = jnp.bfloat16


def remote(src, dst, send, recv, axis, target):
    return pltpu.make_async_remote_copy(
        src_ref=src,
        dst_ref=dst,
        send_sem=send,
        recv_sem=recv,
        device_id={axis: target},
        device_id_type=MESH,
    )


def span(index, size):
    return pl.ds(pl.multiple_of(index * size, size), size)


def loop(low, high, body, **options):
    def step(i, carry):
        body(i)
        return carry

    lax.fori_loop(low, high, step, 0, **options)


def layer_kernel(n, bits, *refs):
    routes, both_in, g_in, u_in, d_in = refs[:5]
    top = routes.shape[1]
    x_in, dy_in = both_in.at[0], both_in.at[1]
    refs = (None, None) + refs
    in_grad, comb_grad, both_out, down_out = refs[7:11]
    x_all, dy_all, x_t, wg, wu, wd, slope, act_all = refs[11:19]
    h_all, h_t, pair_d, hid, rows_out, rows_got = refs[19:25]
    tables, comb_out, comb_got, h_guest, down_guest = refs[25:30]
    both_part, down_part = refs[30:32]
    both_got, down_got = refs[32 : 32 + bits], refs[32 + bits : 32 + 2 * bits]
    rest = refs[32 + 2 * bits :]
    load, a_send, a_recv, t_send, t_recv, r_send, r_recv, c_send, c_recv = rest[:9]
    b_send, b_recv, d_send, d_recv, f_send, f_recv, h_send, h_recv = rest[9:17]

    me = lax.axis_index("expert")
    rank = lax.axis_index("dp")
    replicas = 1 << bits
    half = replicas // 2
    rows = in_grad.shape[0]
    feature, width = wg.shape
    piece = feature // PIECES
    chunks = 2 * width // TILE
    both_rows, down_rows = both_out.shape[0], down_out.shape[0]
    bit = [lax.rem(rank // (1 << b), 2) for b in range(bits)]
    mate = [rank + (1 - 2 * bit[b]) * (1 << b) for b in range(bits)]
    orders = ([0] + list(range(1, bits)), [0] + list(range(bits - 1, 0, -1)))
    is_end = jnp.logical_or(me == 0, me == n - 1)
    is_mid = jnp.logical_not(is_end)

    loads = [
        pltpu.make_async_copy(src, dst, load.at[i])
        for i, (src, dst) in enumerate(
            (
                (g_in.at[0], wg),
                (u_in.at[0], wu),
                (d_in.at[0], wd),
            )
        )
    ]
    barrier = pltpu.get_barrier_semaphore()
    for k in range(1, n):
        pl.semaphore_signal(
            barrier, inc=1, device_id={"expert": lax.rem(me + k, n)}, device_id_type=MESH
        )
    for b in range(bits):
        pl.semaphore_signal(barrier, inc=1, device_id={"dp": mate[b]}, device_id_type=MESH)
    for item in loads:
        item.start()

    weight = routes[1, 0]
    for k in range(1, top):
        weight = weight + routes[1, k]
    tables[me] = weight

    def view(p, block):
        if p is None:
            return x_all.at[span(block, rows)]
        return dy_all.at[span(block, rows), span(p, piece)]

    def index(p):
        return 0 if p is None else 1 + p

    def hop(p, side, s, own=False):
        step = 1 - 2 * side
        block = jnp.clip(me - step * s, 0, n - 1)
        slot = view(p, block)
        target = jnp.clip(me + step, 0, n - 1)
        i = index(p)
        src = slot
        if own:
            src = x_in if p is None else dy_in.at[:, span(p, piece)]
        return remote(src, slot, a_send.at[side, s], a_recv.at[i, block], "expert", target)

    def arrival(p, side, s):
        step = 1 - 2 * side
        block = jnp.clip(me - step * (s + 1), 0, n - 1)
        slot = view(p, block)
        return remote(slot, slot, a_send.at[side, s], a_recv.at[index(p), block], "expert", me)

    def hops(side, s):
        slot = x_all.at[pl.ds(0, 2 * rows)]
        return remote(slot, slot, a_send.at[side, s], a_recv.at[0, 0], "expert", me)

    def sends(side, s):
        if side == 0:
            return jnp.logical_and(me >= s, me + 1 < n)
        return jnp.logical_and(me + s < n, me >= 1)

    def passes(side):
        return jnp.where(side == 0, me + 1 < n, me >= 1)

    def table_copy(target):
        return remote(
            tables.at[me], tables.at[me], t_send.at[0], t_recv.at[me], "expert", target
        )

    def row_copy(target):
        return remote(
            rows_out.at[target],
            rows_got.at[me],
            r_send.at[target],
            r_recv.at[me],
            "expert",
            target,
        )

    def tile_copy(target, j):
        cols = span(j, WIDE)
        return remote(
            rows_out.at[target, :, cols],
            rows_got.at[me, :, cols],
            r_send.at[target],
            r_recv.at[me],
            "expert",
            target,
        )

    fold = n == 4
    ally = n - 1 - me
    near = jnp.where(2 * me < n, 0, n - 1)
    far = n - 1 - near

    shared = PIECES - 1 if fold else PIECES
    helper = jnp.where(me == 0, 1, n - 2)
    own_down = PIECES
    if fold:
        own_down = jnp.where(is_end, shared, PIECES + 1)

    def hidden_copy(b):
        cols = span(b, rows)
        return remote(
            h_t.at[:, cols], h_guest.at[:, cols], h_send.at[0], h_recv.at[0], "expert", helper
        )

    def guest_copy():
        return remote(
            down_guest,
            down_out.at[:, span(PIECES - 1, piece)],
            f_send.at[1],
            f_recv.at[1],
            "expert",
            near,
        )

    def fold_copy():
        return remote(
            rows_out.at[far], rows_got.at[ally], f_send.at[0], f_recv.at[0], "expert", ally
        )

    def folded():
        slot = rows_got.at[me]
        return remote(slot, slot, f_send.at[0], f_recv.at[0], "expert", me)

    def comb_copy(target):
        return remote(
            comb_out.at[target],
            comb_got.at[me],
            c_send.at[0],
            c_recv.at[0],
            "expert",
            target,
        )

    def few(ref, send, recv):
        slot = ref.at[pl.ds(0, n - 1)]
        return remote(slot, slot, send.at[0], recv.at[0], "expert", me)

    pl.semaphore_wait(barrier, n - 1 + bits)
    others = [lax.rem(me + k, n) for k in range(1, n)]
    for target in others:
        table_copy(target).start()
    for p in [None] + list(range(PIECES)):
        for side in range(2):
            ready = sends(side, 0)
            if p is not None and p > 0:
                ready = jnp.logical_and(ready, me == (0, n - 1)[side])

            @pl.when(ready)
            def _():
                hop(p, side, 0, True).start()

    x_all[span(me, rows), :] = x_in[...]
    dy_all[span(me, rows), :] = dy_in[...]
    for item in loads:
        item.wait()

    def coefficient(b):
        line = tables[b, pl.ds(me, 1), :]
        return jnp.broadcast_to(line, (128, rows)).T[:, 0:1]

    def forward(b):
        own = span(b, rows)
        coef = coefficient(b)

        def tile(j):
            cols = span(j, TILE)
            value = x_all[own, :]
            gate = jnp.dot(value, wg[:, cols], preferred_element_type=F32)
            up = jnp.dot(value, wu[:, cols], preferred_element_type=F32)
            sig = jax.nn.sigmoid(gate)
            act = gate * sig
            hidden = (act * up).astype(BF16)
            slope[own, cols] = up * (sig * (1.0 + gate * (1.0 - sig)))
            act_all[own, cols] = act
            h_all[own, cols] = hidden
            h_t[cols, own] = (coef * hidden.astype(F32)).T.astype(BF16)

        loop(0, width // TILE, tile, unroll=True)

        def turn(j):
            cols = span(j, TILE)
            x_t[cols, own] = x_all[own, cols].T

        if fold:

            @pl.when(is_end)
            def _():
                hidden_copy(b).start()

        loop(0, feature // TILE, turn)

    def gather_hidden(b, q, slot=0):
        cols = span(q, piece)
        hid[slot] += lax.dot_general(
            dy_all[span(b, rows), cols], wd[:, cols], LAST, preferred_element_type=F32
        )

    def slopes(b, slot=0):
        own = span(b, rows)
        coef = coefficient(b)

        def tile(j, total):
            cols = span(j, TILE)
            grad = hid[slot, :, cols]
            total = total + jnp.sum(h_all[own, cols].astype(F32) * grad, axis=1, keepdims=True)
            grad = coef * grad
            pair_d[own, cols] = (grad * slope[own, cols]).astype(BF16)
            pair_d[own, span(width // TILE + j, TILE)] = (grad * act_all[own, cols]).astype(BF16)
            return total

        total = lax.fori_loop(0, width // TILE, tile, jnp.zeros((rows, 1), F32), unroll=True)
        comb_out[b] = jnp.broadcast_to(total, (rows, 128)).T[:8]

    def input_tile(b, j):
        own = span(b, rows)
        cols = span(j, WIDE)
        value = lax.dot_general(pair_d[own, :width], wg[cols, :], LAST, preferred_element_type=F32)
        value = value + lax.dot_general(
            pair_d[own, width:], wu[cols, :], LAST, preferred_element_type=F32
        )
        rows_out[b, :, cols] = value.astype(BF16)

    def send_rows(b):
        row_copy(b).start()
        comb_copy(b).start()

    def first(d):
        return jnp.where(jnp.logical_or(d == 0, me >= d), 0, 1)

    def bound(d):
        return jnp.where(jnp.logical_and(d > 0, me + d < n), 2, 1)

    def source(side, d):
        return jnp.clip(me + d * (2 * side - 1), 0, n - 1)

    def by_end(side):
        return jnp.where(side == 0, me == n - 2, me == 1)

    def back(b, d):
        hid[0] = jnp.zeros(hid.shape[1:], F32)
        loop(0, PIECES, lambda q: gather_hidden(b, q))
        slopes(b)
        loop(0, feature // WIDE, functools.partial(input_tile, b))

        @pl.when(jnp.logical_and(is_end, d > 0))
        def _():
            send_rows(b)

    def distance(d):
        def take(side):
            @pl.when(d > 0)
            def _():
                arrival(None, side, d - 1).wait_recv()
                b = source(side, d)
                remote(
                    tables.at[b], tables.at[b], t_send.at[0], t_recv.at[b], "expert", me
                ).wait_recv()

                @pl.when(passes(side))
                def _():
                    hop(None, side, d).start()

                    @pl.when(d == 1)
                    def _():
                        for p in range(1, PIECES):
                            hop(p, side, 0, True).start()

        loop(first(d), bound(d), take)
        loop(first(d), bound(d), lambda side: forward(source(side, d)))
        e = jnp.maximum(d - 1, 0)

        def take_piece(i):
            q, side = i // 2, lax.rem(i, 2)
            here = jnp.logical_and(side >= first(e), side < bound(e))

            @pl.when(jnp.logical_and(here, e > 0))
            def _():
                arrival(q, side, e - 1).wait_recv()
                later = jnp.logical_and(by_end(side), e == n - 3)

                @pl.when(jnp.logical_and(passes(side), jnp.logical_not(later)))
                def _():
                    hop(q, side, e).start()

        @pl.when(jnp.logical_or(d == 0, jnp.logical_and(d > 1, d < n - 1)))
        def _():
            loop(0, 2 * PIECES, take_piece)
            loop(first(e), bound(e), lambda side: back(source(side, e), e))

    loop(0, n, distance)

    @pl.when(jnp.logical_or(me == 1, me == n - 2))
    def _():
        side = jnp.where(me == 1, 1, 0)

        def take(q):
            arrival(q, side, n - 3).wait_recv()
            hop(q, side, n - 3).start()
            hop(q, side, n - 2).start()

        loop(0, PIECES, take)
        back(source(side, n - 2), n - 2)

    if fold:

        @pl.when(is_mid)
        def _():
            fold_copy().start()
            send_rows(ally)

    else:
        for target in others:
            inner = jnp.logical_and(target > 0, target < n - 1)

            @pl.when(jnp.logical_and(is_mid, inner))
            def _():
                send_rows(target)

    def place_of(way, who):
        value = 0
        for i, b in enumerate(orders[way]):
            value = value + lax.rem(who // (1 << b), 2) * (1 << (bits - 1 - i))
        return value

    kinds = {
        "both": (both_part, both_got, b_send, b_recv),
        "down": (down_part, down_got, d_send, d_recv),
    }

    def base(way, i):
        value = 0
        for j in range(i):
            value = value + bit[orders[way][j]] * (replicas >> (j + 1))
        return value

    def stage(kind, c, way, i):
        part, got, send, recv = kinds[kind]
        b = orders[way][i]
        count = replicas >> (i + 1)
        start = base(way, i) + (1 - bit[b]) * count
        pick = slice(None) if i == 0 else way
        return remote(
            part.at[c, pick, pl.ds(start, count)],
            got[i].at[c, pick],
            send.at[0 if kind == "both" else c],
            recv.at[c, i],
            "dp",
            mate[b],
        )

    def staged(kind, c):
        part, _, send, recv = kinds[kind]
        slot = part.at[c, :, pl.ds(0, replicas - 1)]
        return remote(slot, slot, send.at[0 if kind == "both" else c], recv.at[0, 0], "dp", rank)

    def combine(kind, c, i):
        part, got, _, _ = kinds[kind]
        count = replicas >> (i + 1)
        recv = kinds[kind][3]
        slot = got[i].at[c]
        remote(slot, slot, kinds[kind][2].at[0], recv.at[c, i], "dp", rank).wait_recv()
        for way in range(2):
            start = base(way, i + 1)
            if i == bits - 1:
                total = part[c, way, start].astype(F32) + got[i][c, way, 0].astype(F32)
                if kind == "both":
                    both_out[:, span(2 * c + way, TILE // 2)] = total.astype(BF16)
                elif fold:

                    @pl.when(c < PIECES)
                    def _():
                        down_out[:, span(2 * c + way, piece // 2)] = total.astype(BF16)

                    @pl.when(c == PIECES)
                    def _():
                        down_guest[:, span(way, piece // 2)] = total.astype(BF16)

                else:
                    down_out[:, span(2 * c + way, piece // 2)] = total.astype(BF16)
                continue

            def add(k):
                total = part[c, way, start + k].astype(F32) + got[i][c, way, k].astype(F32)
                part[c, way, start + k] = total.astype(BF16)

            loop(0, count, add, unroll=min(count, 4))
            stage(kind, c, way, i + 1).start()

    def spread(kind, c, who, value):
        part = kinds[kind][0]
        size = value.shape[1] // 2
        for way in range(2):
            half_value = value[:, way * size : (way + 1) * size]
            part[c, way, place_of(way, who)] = half_value.astype(BF16)

    def both_chunk(c):
        def place(side, j):
            who = 2 * j + side
            lines = span(who, both_rows)
            value = jnp.dot(x_t[lines, :], pair_d[:, span(c, TILE)], preferred_element_type=F32)
            spread("both", c, who, value)

        loop(0, half, functools.partial(place, 1 - bit[0]), unroll=2)
        stage("both", c, 0, 0).start()
        loop(0, half, functools.partial(place, bit[0]), unroll=2)

    def down_chunk(q, held=h_t):
        cols = span(min(q, PIECES - 1) if isinstance(q, int) else q, piece)
        group = 1 if down_rows % 16 == 0 else 2

        def place(side, j):
            who = 2 * j + side
            lines = span(who // group, group * down_rows)
            value = jnp.dot(held[lines, :], dy_all[:, cols], preferred_element_type=F32)
            for k in range(group):
                spread("down", q, who + k, value[k * down_rows : (k + 1) * down_rows])

        if group == 1:
            loop(0, half, functools.partial(place, 1 - bit[0]), unroll=2)
            stage("down", q, 0, 0).start()
            loop(0, half, functools.partial(place, bit[0]), unroll=2)
        else:
            loop(0, half, functools.partial(place, 0))
            stage("down", q, 0, 0).start()

    last = jnp.clip(n - 1 - me, 0, n - 1)
    prior = jnp.where(me == n - 1, 1, n - 2)
    last_side = jnp.where(me == n - 1, 0, 1)

    @pl.when(is_end)
    def _():
        hid[...] = jnp.zeros_like(hid)

    wide = feature // WIDE

    def last_tile(j):
        @pl.when(jnp.logical_and(is_end, j < 2 * wide))
        def _():
            b = jnp.where(j < wide, last, prior)
            tile = lax.rem(j, wide)
            input_tile(b, tile)
            tile_copy(b, tile).start()

            @pl.when(tile == wide - 1)
            def _():
                comb_copy(b).start()

    def early(q):
        @pl.when(is_end)
        def _():
            for slot, b in enumerate((prior, last)):
                arrival(q, last_side, n - 3 + slot).wait_recv()
                gather_hidden(b, q, slot)

        down_chunk(q)
        combine("down", q, 0)

        @pl.when(q > 0)
        def _():
            combine("down", q - 1, 1)

    loop(0, PIECES - 1, early)

    @pl.when(is_end)
    def _():
        for slot, b in enumerate((prior, last)):
            arrival(PIECES - 1, last_side, n - 3 + slot).wait_recv()
            gather_hidden(b, PIECES - 1, slot)
            slopes(b, slot)

    if fold:

        @pl.when(is_mid)
        def _():
            remote(h_guest, h_guest, h_send.at[0], h_recv.at[0], "expert", me).wait_recv()
            down_chunk(PIECES, h_guest)

    both_chunk(0)
    both_chunk(1)
    combine("both", 0, 0)
    combine("down", PIECES - 2, 1)
    last_tile(0)
    combine("both", 1, 0)

    def rest_down(i):
        if i == 0:
            down_chunk(PIECES - 1)
            if fold:
                combine("down", PIECES, 0)
        combine("down", PIECES - 1, i)
        if fold and i > 0:
            combine("down", PIECES, i)

    def when_owned(body):
        if fold:
            pl.when(is_mid)(body)
        else:
            body()

    when_owned(lambda: rest_down(0))
    last_tile(1)
    last_tile(2)

    def settle():
        for side in range(2):
            for s in range(n - 1):

                @pl.when(sends(side, s))
                def _():
                    hops(side, s).wait_send()

        if fold:

            @pl.when(is_mid)
            def _():
                folded().wait_recv()

                def add(j):
                    cols = span(j, TILE)
                    total = rows_out[near, :, cols].astype(F32) + rows_got[me, :, cols].astype(F32)
                    rows_out[near, :, cols] = total.astype(BF16)

                loop(0, feature // TILE, add)
                row_copy(near).start()
                comb_copy(near).start()
                comb_copy(far).start()

        else:
            for target in others:
                outer = jnp.logical_or(target == 0, target == n - 1)

                @pl.when(jnp.logical_and(is_mid, outer))
                def _():
                    send_rows(target)

    def late(c):
        both_chunk(c)
        for t in range(2):
            last_tile(2 * c - 1 + t)
        combine("both", c, 0)

        @pl.when(c == 3)
        def _():
            when_owned(lambda: rest_down(1))

        @pl.when(c == 2)
        def _():
            settle()

    loop(2, chunks, late)

    for i in range(1, bits - 1):
        if i > 1:
            loop(0, own_down, lambda q: combine("down", q, i))
        loop(0, chunks, lambda c: combine("both", c, i))

    loop(0, own_down, lambda q: combine("down", q, bits - 1))
    if fold:

        @pl.when(is_mid)
        def _():
            guest_copy().start()


    def takes_row(b):
        if not fold:
            return b >= 0
        return jnp.logical_or(is_mid, b != jnp.where(me == 0, n - 2, 1))

    def gives_row(target):
        if not fold:
            return target >= 0
        return jnp.logical_or(is_end, target != far)

    for b in others:

        @pl.when(takes_row(b))
        def _():
            remote(
                rows_got.at[b], rows_got.at[b], r_send.at[b], r_recv.at[b], "expert", me
            ).wait_recv()


    few(comb_got, c_send, c_recv).wait_recv()

    def total_rows(who):
        def tile(j):
            cols = span(j, TILE)
            total = rows_out[me, :, cols].astype(F32)
            for b in who:
                total = total + rows_got[b, :, cols].astype(F32)
            in_grad[:, cols] = total.astype(BF16)

        loop(0, feature // TILE, tile)

    if fold:

        @pl.when(is_end)
        def _():
            total_rows([n - 1 - me, jnp.where(me == 0, 1, n - 2)])

        @pl.when(is_mid)
        def _():
            total_rows(others)

    else:
        total_rows(others)

    for k in range(top):

        def pick(b, line):
            return jnp.where(routes[0, k, pl.ds(b, 1), :] > 0.5, line, 0.0)

        picked = pick(me, comb_out[me, 0:1, :])
        for b in others:
            picked = picked + pick(b, comb_got[b, 0:1, :])
        comb_grad[k : k + 1, :] = picked

    if fold:

        @pl.when(is_end)
        def _():
            slot = down_out.at[:, span(PIECES - 1, piece)]
            remote(slot, slot, f_send.at[1], f_recv.at[1], "expert", me).wait_recv()
            remote(h_t, h_t, h_send.at[0], h_recv.at[0], "expert", me).wait_send()

        @pl.when(is_mid)
        def _():
            guest_copy().wait_send()

    few(tables, t_send, t_recv).wait_send()
    few(comb_out, c_send, c_recv).wait_send()
    for target in others:

        @pl.when(gives_row(target))
        def _():
            row_copy(target).wait_send()

    if fold:

        @pl.when(is_mid)
        def _():
            fold_copy().wait_send()

    loop(0, own_down, lambda q: staged("down", q).wait_send())

    loop(0, chunks, lambda c: combine("both", c, bits - 1))
    staged("both", slice(None)).wait_send()


def deliver_kernel(rows, comb, both, down, *refs):
    outs, sems = refs[:-1], refs[-1]
    width = outs[2].shape[2]
    copies = []
    for src, dst in (
        (rows, outs[0]),
        (both.at[:, pl.ds(0, width)], outs[2].at[0]),
        (both.at[:, pl.ds(width, width)], outs[3].at[0]),
        (down, outs[4].at[0]),
        (comb, outs[1]),
    ):
        copies.append(pltpu.make_async_copy(src, dst, sems.at[len(copies)]))
        copies[-1].start()
    for copy in copies:
        copy.wait()


def deliver(rows, comb, both, down):
    width = both.shape[1] // 2
    outs = [
        jax.ShapeDtypeStruct(rows.shape, BF16),
        jax.ShapeDtypeStruct(comb.shape, F32),
        jax.ShapeDtypeStruct((1, both.shape[0], width), BF16),
        jax.ShapeDtypeStruct((1, both.shape[0], width), BF16),
        jax.ShapeDtypeStruct((1,) + down.shape, BF16),
    ]
    input_grad, combine_grad, gate_grad, up_grad, down_grad = pl.pallas_call(
        deliver_kernel,
        out_shape=outs,
        in_specs=[VMEM] * 4,
        out_specs=[HBM] * 5,
        scratch_shapes=[pltpu.SemaphoreType.DMA((5,))],
        compiler_params=pltpu.CompilerParams(vmem_limit_bytes=8 * 1024 * 1024),
        name="deliver",
    )(rows, comb, both, down)
    return (input_grad, combine_grad.T, gate_grad, up_grad, down_grad)


def shards(tokens, cotangent, expert_ids, combine, w_gate, w_up, w_down):
    n = lax.axis_size("expert")
    replicas = lax.axis_size("dp")
    bits = replicas.bit_length() - 1
    rows, top = expert_ids.shape
    feature = tokens.shape[1]
    width = w_gate.shape[2]
    everyone = n * rows
    chunks = 2 * width // TILE
    piece = feature // PIECES
    both_rows, down_rows = feature // replicas, width // replicas
    table = -(-n // 8) * 8
    outs = [
        jax.ShapeDtypeStruct((rows, feature), BF16),
        jax.ShapeDtypeStruct((top, rows), F32),
        jax.ShapeDtypeStruct((both_rows, 2 * width), BF16),
        jax.ShapeDtypeStruct((down_rows, feature), BF16),
    ]
    scratch = [
        pltpu.VMEM((everyone, feature), BF16),
        pltpu.VMEM((everyone, feature), BF16),
        pltpu.VMEM((feature, everyone), BF16),
        pltpu.VMEM((feature, width), BF16),
        pltpu.VMEM((feature, width), BF16),
        pltpu.VMEM((width, feature), BF16),
        pltpu.VMEM((everyone, width), F32),
        pltpu.VMEM((everyone, width), F32),
        pltpu.VMEM((everyone, width), BF16),
        pltpu.VMEM((width, everyone), BF16),
        pltpu.VMEM((everyone, 2 * width), BF16),
        pltpu.VMEM((2, rows, width), F32),
        pltpu.VMEM((n, rows, feature), BF16),
        pltpu.VMEM((n, rows, feature), BF16),
        pltpu.VMEM((n, table, rows), F32),
        pltpu.VMEM((n, 8, rows), F32),
        pltpu.VMEM((n, 8, rows), F32),
        pltpu.VMEM((width, everyone), BF16),
        pltpu.VMEM((down_rows, piece), BF16),
        pltpu.VMEM((chunks, 2, replicas, both_rows, TILE // 2), BF16),
        pltpu.VMEM((PIECES + 1, 2, replicas, down_rows, piece // 2), BF16),
    ]
    for i in range(bits):
        count = replicas >> (i + 1)
        scratch.append(pltpu.VMEM((chunks, 2, count, both_rows, TILE // 2), BF16))
    for i in range(bits):
        count = replicas >> (i + 1)
        scratch.append(pltpu.VMEM((PIECES + 1, 2, count, down_rows, piece // 2), BF16))
    scratch += [pltpu.SemaphoreType.DMA((3,))]
    for shape in ((2, n - 1), (1 + PIECES, n), (1,), (n,), (n,), (n,), (1,), (1,)):
        scratch.append(pltpu.SemaphoreType.DMA(shape))
    for one, count in ((1, chunks), (PIECES + 1, PIECES + 1)):
        scratch += [pltpu.SemaphoreType.DMA((one,)), pltpu.SemaphoreType.DMA((count, bits))]
    scratch += [pltpu.SemaphoreType.DMA((2,))] * 2
    scratch += [pltpu.SemaphoreType.DMA((1,))] * 2
    names = lax.broadcasted_iota(jnp.int32, (2, top, table, rows), 2)
    kind = lax.broadcasted_iota(jnp.int32, (2, top, table, rows), 0)
    value = jnp.where(kind == 0, 1.0, combine.T[None, :, None, :])
    routes = jnp.where(names == expert_ids.T[None, :, None, :], value, 0.0)
    input_grad, combine_grad, both, down = pl.pallas_call(
        functools.partial(layer_kernel, n, bits),
        out_shape=outs,
        in_specs=[VMEM] * 2 + [HBM] * 3,
        out_specs=[VMEM] * 4,
        scratch_shapes=scratch,
        compiler_params=pltpu.CompilerParams(
            collective_id=0, has_side_effects=True, vmem_limit_bytes=LIMIT
        ),
        name="layer",
    )(routes, jnp.stack([tokens, cotangent]), w_gate, w_up, w_down)
    return deliver(input_grad, combine_grad, both, down)


def solution(mesh):
    by_token = P(("dp", "expert"), None)
    by_expert = P("expert", None, None)
    by_row = P("expert", "dp", None)
    return jax.shard_map(
        shards,
        mesh=mesh,
        in_specs=(by_token,) * 4 + (by_expert,) * 3,
        out_specs=(by_token, by_token, by_row, by_row, by_row),
        check_vma=False,
    )
```
